32 devices in a mesh: lat: 8 (over y, x, core), rad: 4 (over z).
Axes of the slice: x: 2, y: 2, z: 4, core: 2. Of those that a mesh axis runs over, the one named last changes fastest.
Arguments:
- schur_off: bfloat16 [8, 4, 1536, 1536], P('lat', 'rad'), may hold values from -0.15625 to 0.15625
- schur_diag: float32 [8, 4, 1536], P('lat', 'rad'), may hold values from 1.5 to 4
- source: float32 [8, 4, 1536, 128], P('lat', 'rad'), may hold values from -6 to 6
- start: float32 [8, 4, 1536, 128], P('lat', 'rad'), may hold values from -6 to 6
- decay: float32 [8, 4, 256, 128], P('lat', 'rad'), may hold values from 0.2 to 1
- neighbour_face: int32 [8, 4], replicated, may hold values from 0 to 3
- orientation: int32 [8, 4], replicated, may hold values from 0 to 7
Outputs:
- traces: float32 [8, 4, 1536, 128], P('lat', 'rad')
The draws below stay inside these ranges and needn't reach their ends.
Inputs may be any that keep to these rules, and one draw needn't show every extreme that they name: `neighbour_face`: a face index of 0 to 3. `orientation`: a code of 0 to 7 whose bits select transpose, row reflection and column reflection.
All inputs are finite; a program needn't handle non-finite values.
Results may differ from the reference program's by a relative error of at most 0.001.
Values sent between devices are 32-bit elements; how exact they have to be, the bound alone decides.
A program may use at most 64 MiB of HBM per device.

```python
import math
import jax
import jax.numpy as jnp
import numpy as np
from jax import lax

FACE_SIDE = 16
FACE_NODES = 256
ORDER = 1536
COLS = 128
ITERS = 2
RADIAL_PASSES = 2
FAR = 2
N_LAT = 8
N_RAD = 4


def plant(array, stream_key, low, top_value):
    extent = array.shape
    place = [jax.random.randint(jax.random.fold_in(stream_key, axis), (), 0, extent[axis]) for axis in range(len(extent))]
    array = array.at[tuple(place)].set(low)
    longest = extent.index(max(extent))
    place[longest] = (place[longest] + 1) % extent[longest]
    return array.at[tuple(place)].set(top_value)


def steps_of(key, extent, cuts, smallest, largest):
    def one(dim, blocks):
        draws = jax.random.uniform(jax.random.fold_in(jax.random.fold_in(key, 6), dim), (blocks,), jnp.float32, smallest / len(cuts), largest / len(cuts))
        return jnp.repeat(jnp.exp(draws), extent[dim] // blocks).reshape((-1,) + (1,) * (len(extent) - dim - 1))

    gain = one(*cuts[0])
    for cut in cuts[1:]:
        gain = gain * one(*cut)
    return gain


def gaussian(own_key, extent, width, limit, shards=(), dtype=jnp.bfloat16):
    entries = jax.random.normal(own_key, extent, jnp.float32) * width
    if len(shards) > 0:
        entries = steps_of(own_key, extent, shards, -0.22, 0.18) * entries
    return jnp.clip(entries, min=-limit, max=limit).astype(dtype)


def setup_inputs(seed: int = 0) -> dict:
    seeds = jax.random.split(jax.random.key(seed), 8)
    return {
        "schur_off": gaussian(seeds[0], (N_LAT, N_RAD, ORDER, ORDER), ORDER ** -0.5, 0.15625, ((0, 8), (1, 4))),
        "schur_diag": jnp.clip(jnp.exp(math.log(4.0) - 0.98082925 * jax.random.uniform(seeds[1], (N_LAT, N_RAD, ORDER), jnp.float32) ** steps_of(seeds[1], (N_LAT, N_RAD, ORDER), ((0, 8), (1, 4)), -0.2, 0.2)), 1.5, 4.0),
        "source": gaussian(seeds[2], (N_LAT, N_RAD, ORDER, COLS), 1.0, 6.0, ((0, 8), (1, 4)), jnp.float32),
        "start": gaussian(seeds[3], (N_LAT, N_RAD, ORDER, COLS), 1.0, 6.0, ((0, 8), (1, 4)), jnp.float32),
        "decay": jnp.clip(0.2 + 0.8 * jax.random.uniform(seeds[4], (N_LAT, N_RAD, FACE_NODES, COLS), jnp.float32) ** steps_of(seeds[4], (N_LAT, N_RAD, FACE_NODES, COLS), ((0, 8), (1, 4)), -0.2, 0.2), 0.2, 1.0),
        "neighbour_face": plant(jax.random.randint(seeds[5], (N_LAT, 4), 0, 4), jax.random.fold_in(seeds[5], 1), 0, 3).astype(jnp.int32),
        "orientation": plant(jax.random.randint(seeds[6], (N_LAT, 4), 0, 8), jax.random.fold_in(seeds[6], 1), 0, 7).astype(jnp.int32),
    }


OMEGA = 0.3
COUPLE = 0.5


def orient_table(side):
    table = np.zeros((8, side * side), np.int32)
    for code in range(8):
        for i in range(side):
            for j in range(side):
                first, second = (j, i) if code & 1 else (i, j)
                if code & 2:
                    first = side - 1 - first
                if code & 4:
                    second = side - 1 - second
                table[code, i * side + j] = first * side + second
    return table


def apply_block(schur_off, schur_diag, trace):
    flat_w = schur_off.reshape(-1, ORDER, ORDER)
    flat_d = schur_diag.reshape(-1, ORDER)
    flat_u = trace.reshape(-1, ORDER, COLS)

    def single(items):
        weight, diag, value = items
        return jnp.dot(weight, value.astype(jnp.bfloat16), preferred_element_type=jnp.float32) + diag[:, None] * value

    return lax.map(single, (flat_w, flat_d, flat_u)).reshape(trace.shape)


def reference(schur_off, schur_diag, source, start, decay, neighbour_face, orientation):
    table = jnp.asarray(orient_table(FACE_SIDE))
    offsets = (-1, 1, -FAR, FAR)
    trace = start
    blank = jnp.zeros((N_LAT, N_RAD, FACE_NODES, COLS), jnp.float32)
    for outer in range(ITERS):
        applied = apply_block(schur_off, schur_diag, trace)
        faces = trace.reshape(N_LAT, N_RAD, 6, FACE_NODES, COLS)[:, :, :4]
        incoming = []
        for k in range(4):
            beside = jnp.roll(faces, -offsets[k], axis=0)
            pick = jnp.take_along_axis(beside, neighbour_face[:, k][:, None, None, None, None].astype(jnp.int32), axis=2)[:, :, 0]
            perm = table[orientation[:, k]]
            incoming.append(jnp.take_along_axis(pick, perm[:, None, :, None].astype(jnp.int32), axis=2))
        coupling = jnp.stack(incoming + [blank, blank], axis=2).reshape(trace.shape)
        trace = trace + OMEGA * (source - applied + COUPLE * coupling)
        for sweep in range(RADIAL_PASSES):
            res = source - apply_block(schur_off, schur_diag, trace)
            parts = res.reshape(N_LAT, N_RAD, 6, FACE_NODES, COLS)
            top = parts[:, :, 5]
            bottom = parts[:, :, 4]
            carry = jnp.zeros((N_LAT, FACE_NODES, COLS), jnp.float32)
            inflows = []
            for layer in range(N_RAD):
                inflows.append(carry)
                carry = decay[:, layer] * (carry + top[:, layer])
            inflow = jnp.stack(inflows, axis=1)
            above = jnp.concatenate([bottom[:, 1:], blank[:, :1]], axis=1)
            coupling = jnp.stack([blank, blank, blank, blank, inflow, above], axis=2).reshape(trace.shape)
            trace = trace + OMEGA * (res + COUPLE * coupling)
    return trace
```

```python
import functools
import math

import jax
import jax.numpy as jnp
from jax import lax
from jax.experimental import pallas as pl
from jax.experimental.pallas import tpu as pltpu
from jax.sharding import PartitionSpec as P

ITERS = 2
RADIAL_PASSES = 2
OMEGA = 0.3
COUPLE = 0.5
CHUNKS = 8
SEND_ORDER = (2, 3, 0, 1)
MESH = pl.DeviceIdType.MESH


def permuted(face, code, side):
    nodes = side * side
    n = lax.broadcasted_iota(jnp.int32, (nodes, 1), 0)
    i, j = n // side, n % side
    swap, rows, cols = code & 1, (code >> 1) & 1, (code >> 2) & 1
    a = i + swap * (j - i)
    b = j + swap * (i - j)
    a = a + rows * (side - 1 - 2 * a)
    b = b + cols * (side - 1 - 2 * b)
    at = lax.broadcasted_iota(jnp.int32, (nodes, nodes), 1)
    hot = jnp.where(at == a * side + b, 1.0, 0.0).astype(jnp.bfloat16)
    high = face.astype(jnp.bfloat16)
    rest = face - high.astype(jnp.float32)
    middle = rest.astype(jnp.bfloat16)
    low = (rest - middle.astype(jnp.float32)).astype(jnp.bfloat16)
    total = None
    for part in (low, middle, high):
        moved = jnp.dot(hot, part, preferred_element_type=jnp.float32)
        total = moved if total is None else total + moved
    return total


def kernel(
    lat_count, rad_count, nodes,
    face_at, code_at, diag_ref, w_hbm, source_hbm, start_hbm, decay_hbm,
    out_ref,
    w, ub, rhs, factor, diag, res, ready,
    lat_out, lat_in, dn_out, dn_in, h_out, h_in,
    load_sem, w_sem,
    lat_send, lat_recv, dn_send, dn_recv, h_send, h_recv,
):
    side = math.isqrt(nodes)
    far = max(2, lat_count // 8)
    offsets = (-1, 1, -far, far)
    p = lax.axis_index("lat")
    r = lax.axis_index("rad")
    size = nodes // CHUNKS
    u = out_ref.at[0, 0]
    lanes = u.shape[1]
    upper, lower = slice(0, 4 * nodes), slice(4 * nodes, 6 * nodes)

    load_u = pltpu.make_async_copy(start_hbm.at[0, 0], u, load_sem.at[0])
    load_rhs = pltpu.make_async_copy(source_hbm.at[0, 0], rhs, load_sem.at[1])
    load_factor = pltpu.make_async_copy(decay_hbm.at[0, 0], factor, load_sem.at[2])
    load_w = [
        pltpu.make_async_copy(w_hbm.at[0, 0, part], w.at[part], w_sem.at[n])
        for n, part in enumerate((upper, lower))
    ]
    load_u.start()
    for copy in load_w:
        copy.start()
    load_rhs.start()
    load_factor.start()

    barrier = pltpu.get_barrier_semaphore()
    for offset in offsets:
        target = (p - offset + lat_count) % lat_count
        pl.semaphore_signal(barrier, inc=1, device_id={"lat": target}, device_id_type=MESH)

    below, above = (r - 1 + rad_count) % rad_count, (r + 1) % rad_count

    @pl.when(r > 0)
    def _():
        pl.semaphore_signal(barrier, inc=1, device_id={"rad": below}, device_id_type=MESH)

    @pl.when(r < rad_count - 1)
    def _():
        pl.semaphore_signal(barrier, inc=1, device_id={"rad": above}, device_id_type=MESH)

    inner = (r + rad_count - 1) // rad_count + (2 * rad_count - 2 - r) // rad_count

    def lat_copy(outer, k):
        target = (p - offsets[k] + lat_count) % lat_count
        return pltpu.make_async_remote_copy(
            src_ref=lat_out.at[outer, k], dst_ref=lat_in.at[outer, k],
            send_sem=lat_send.at[outer, k], recv_sem=lat_recv.at[outer, k],
            device_id={"lat": target}, device_id_type=MESH,
        )

    def dn_copy(sweep):
        return pltpu.make_async_remote_copy(
            src_ref=dn_out.at[sweep], dst_ref=dn_in.at[sweep],
            send_sem=dn_send.at[sweep], recv_sem=dn_recv.at[sweep],
            device_id={"rad": below}, device_id_type=MESH,
        )

    def h_copy(sweep, c):
        rows = pl.ds(c * size, size)
        return pltpu.make_async_remote_copy(
            src_ref=h_out.at[sweep, rows], dst_ref=h_in.at[sweep, rows],
            send_sem=h_send.at[sweep, c], recv_sem=h_recv.at[sweep, c],
            device_id={"rad": above}, device_id_type=MESH,
        )

    def make_faces(outer, which_faces):
        for k in which_faces:
            target = (p - offsets[k] + lat_count) % lat_count
            which = jnp.full((nodes, lanes), face_at[k, target], jnp.int32)
            face = u[slice(0, nodes), :]
            for f in range(1, 4):
                face = jnp.where(which == f, u[slice(f * nodes, (f + 1) * nodes), :], face)
            lat_out[outer, k] = permuted(face, code_at[k, target], side)

    def start_faces(outer, which_faces):
        for k in which_faces:
            lat_copy(outer, k).start()

    def residual(part):
        applied = jnp.dot(w[part, :], ub[...], preferred_element_type=jnp.float32)
        return rhs[part, :] - (applied + diag[part, :] * u[part, :])

    load_u.wait()
    make_faces(0, SEND_ORDER[:2])
    pl.semaphore_wait(barrier, len(offsets) + inner)
    start_faces(0, SEND_ORDER[:2])
    for k in SEND_ORDER[2:]:
        make_faces(0, (k,))
        start_faces(0, (k,))
    ub[...] = u[...].astype(jnp.bfloat16)
    for block in range(6 * nodes // lanes):
        own = slice(block * lanes, (block + 1) * lanes)
        diag[own, :] = jnp.broadcast_to(diag_ref[0, :, own], (lanes, lanes)).T
    load_rhs.wait()
    load_factor.wait()
    for copy in load_w:
        copy.wait()

    for outer in range(ITERS):
        for part in (upper, lower):
            res[part, :] = residual(part)
        u[lower, :] = u[lower, :] + OMEGA * res[lower, :]
        ub[lower, :] = u[lower, :].astype(jnp.bfloat16)
        ready[...] = jnp.dot(w[lower, lower], ub[lower, :], preferred_element_type=jnp.float32)
        for k in SEND_ORDER:
            own = slice(k * nodes, (k + 1) * nodes)
            lat_copy(outer, k).wait_recv()
            new = u[own, :] + OMEGA * (res[own, :] + COUPLE * lat_in[outer, k])
            u[own, :] = new
            ub[own, :] = new.astype(jnp.bfloat16)
            if k != SEND_ORDER[-1]:
                ready[...] = ready[...] + jnp.dot(
                    w[lower, own], ub[own, :], preferred_element_type=jnp.float32
                )
        for turn in range(RADIAL_PASSES):
            sweep = outer * RADIAL_PASSES + turn
            bottom = slice(4 * nodes, 5 * nodes)
            top = slice(5 * nodes, 6 * nodes)
            last = slice(SEND_ORDER[-1] * nodes, (SEND_ORDER[-1] + 1) * nodes) if turn == 0 else lower
            applied = ready[...] + jnp.dot(
                w[lower, last], ub[last, :], preferred_element_type=jnp.float32
            )
            res[lower, :] = rhs[lower, :] - (applied + diag[lower, :] * u[lower, :])

            @pl.when(r > 0)
            def _():
                dn_out[sweep] = res[bottom, :]
                dn_copy(sweep).start()

            @pl.when(r == 0)
            def _():
                h_out[sweep] = factor[...] * res[top, :]
                for c in range(CHUNKS):
                    h_copy(sweep, c).start()

            new = u[upper, :] + OMEGA * residual(upper)
            u[upper, :] = new
            ub[upper, :] = new.astype(jnp.bfloat16)
            if turn == RADIAL_PASSES - 1:
                if outer < ITERS - 1:
                    for k in SEND_ORDER:
                        make_faces(outer + 1, (k,))
                        start_faces(outer + 1, (k,))
            else:
                ready[...] = jnp.dot(w[lower, upper], ub[upper, :], preferred_element_type=jnp.float32)

            @pl.when(r > 0)
            def _():
                for c in range(CHUNKS):
                    rows = slice(c * size, (c + 1) * size)
                    from_bottom = slice(4 * nodes + c * size, 4 * nodes + (c + 1) * size)
                    from_top = slice(5 * nodes + c * size, 5 * nodes + (c + 1) * size)
                    h_copy(sweep, c).wait_recv()

                    @pl.when(r < rad_count - 1)
                    def _():
                        h_out[sweep, rows] = factor[rows, :] * (h_in[sweep, rows] + res[from_top, :])
                        h_copy(sweep, c).start()

                    u[from_bottom, :] = u[from_bottom, :] + OMEGA * (
                        res[from_bottom, :] + COUPLE * h_in[sweep, rows]
                    )

            @pl.when(r == 0)
            def _():
                u[bottom, :] = u[bottom, :] + OMEGA * res[bottom, :]

            @pl.when(r < rad_count - 1)
            def _():
                dn_copy(sweep).wait_recv()
                u[top, :] = u[top, :] + OMEGA * (res[top, :] + COUPLE * dn_in[sweep])

            @pl.when(r == rad_count - 1)
            def _():
                u[top, :] = u[top, :] + OMEGA * res[top, :]

            ub[lower, :] = u[lower, :].astype(jnp.bfloat16)

    for outer in range(ITERS):
        for k in SEND_ORDER:
            lat_copy(outer, k).wait_send()

    @pl.when(r > 0)
    def _():
        for sweep in range(ITERS * RADIAL_PASSES):
            dn_copy(sweep).wait_send()

    @pl.when(r < rad_count - 1)
    def _():
        for sweep in range(ITERS * RADIAL_PASSES):
            for c in range(CHUNKS):
                h_copy(sweep, c).wait_send()


def per_device(lat_count, rad_count, schur_off, schur_diag, source, start, decay, neighbour_face, orientation):
    order, columns = source.shape[2:]
    nodes = order // 6
    sweeps = ITERS * RADIAL_PASSES
    faces = lambda *lead: pltpu.VMEM((*lead, nodes, columns), jnp.float32)
    dma = lambda *shape: pltpu.SemaphoreType.DMA(shape)
    smem = pl.BlockSpec(memory_space=pltpu.SMEM)
    vmem = pl.BlockSpec(memory_space=pltpu.VMEM)
    hbm = pl.BlockSpec(memory_space=pl.ANY)
    return pl.pallas_call(
        functools.partial(kernel, lat_count, rad_count, nodes),
        out_shape=jax.ShapeDtypeStruct(source.shape, jnp.float32),
        in_specs=[smem, smem, vmem, hbm, hbm, hbm, hbm],
        out_specs=vmem,
        scratch_shapes=[
            pltpu.VMEM((order, order), jnp.bfloat16),
            pltpu.VMEM((order, columns), jnp.bfloat16),
            pltpu.VMEM((order, columns), jnp.float32),
            faces(),
            pltpu.VMEM((order, columns), jnp.float32),
            pltpu.VMEM((order, columns), jnp.float32),
            pltpu.VMEM((2 * nodes, columns), jnp.float32),
            faces(ITERS, 4), faces(ITERS, 4), faces(sweeps), faces(sweeps), faces(sweeps), faces(sweeps),
            dma(3), dma(2),
            dma(ITERS, 4), dma(ITERS, 4), dma(sweeps), dma(sweeps),
            dma(sweeps, CHUNKS), dma(sweeps, CHUNKS),
        ],
        compiler_params=pltpu.CompilerParams(
            collective_id=0, has_side_effects=True, vmem_limit_bytes=24 * 1024 * 1024
        ),
        name="shell",
    )(*(
        pltpu.with_memory_space_constraint(x, pltpu.HBM)
        for x in (neighbour_face.T, orientation.T, schur_diag, schur_off, source, start, decay)
    ))


def solution(mesh):
    lat_count, rad_count = mesh.shape["lat"], mesh.shape["rad"]
    return jax.shard_map(
        functools.partial(per_device, lat_count, rad_count),
        mesh=mesh,
        in_specs=(
            P("lat", "rad", None, None),
            P("lat", "rad", None),
            P("lat", "rad", None, None),
            P("lat", "rad", None, None),
            P("lat", "rad", None, None),
            P(),
            P(),
        ),
        out_specs=P("lat", "rad", None, None),
        check_vma=False,
    )
```

```python
import contextlib
import functools
import math

import jax
import jax.numpy as jnp
from jax import lax
from jax.experimental import pallas as pl
from jax.experimental.pallas import tpu as pltpu
from jax.sharding import PartitionSpec as P

ITERS = 2
RADIAL_PASSES = 2
OMEGA = 0.3
COUPLE = 0.5
CHUNKS = 8
SEND_ORDER = (2, 3, 0, 1)
MESH = pl.DeviceIdType.MESH


def scope(name):
    return contextlib.nullcontext()


def one_hot(code, side):
    nodes = side * side
    n = lax.broadcasted_iota(jnp.int32, (nodes, 1), 0)
    i, j = n // side, n % side
    swap, rows, cols = code & 1, (code >> 1) & 1, (code >> 2) & 1
    a = i + swap * (j - i)
    b = j + swap * (i - j)
    a = a + rows * (side - 1 - 2 * a)
    b = b + cols * (side - 1 - 2 * b)
    at = lax.broadcasted_iota(jnp.int32, (nodes, nodes), 1)
    return jnp.where(at == a * side + b, 1.0, 0.0).astype(jnp.bfloat16)


def permuted(hot, face):
    high = face.astype(jnp.bfloat16)
    rest = face - high.astype(jnp.float32)
    middle = rest.astype(jnp.bfloat16)
    low = (rest - middle.astype(jnp.float32)).astype(jnp.bfloat16)
    total = None
    for part in (low, middle, high):
        moved = jnp.dot(hot, part, preferred_element_type=jnp.float32)
        total = moved if total is None else total + moved
    return total


def kernel(
    lat_count, rad_count, nodes,
    face_hbm, code_hbm, diag_hbm, w_hbm, source_hbm, start_hbm, decay_hbm,
    out_hbm,
    face_at, code_at, diag_row, w, u, ub, rhs, factor, diag, acc, res_top, hot,
    lat_out, lat_in, dn_out, dn_in, h_out, h_in,
    small_sem, load_sem, w_sem, out_sem,
    lat_send, lat_recv, dn_send, dn_recv, h_send, h_recv,
):
    side = math.isqrt(nodes)
    far = max(2, lat_count // 8)
    offsets = (-1, 1, -far, far)
    p = lax.axis_index("lat")
    r = lax.axis_index("rad")
    size = nodes // CHUNKS
    lanes = u.shape[1]
    upper, lower, every = slice(0, 4 * nodes), slice(4 * nodes, 6 * nodes), slice(0, 6 * nodes)
    bottom, top = slice(4 * nodes, 5 * nodes), slice(5 * nodes, 6 * nodes)

    load_face = pltpu.make_async_copy(face_hbm, face_at, small_sem.at[0])
    load_code = pltpu.make_async_copy(code_hbm, code_at, small_sem.at[1])
    load_diag = pltpu.make_async_copy(diag_hbm.at[0], diag_row, small_sem.at[2])
    load_u = pltpu.make_async_copy(start_hbm.at[0, 0], u, load_sem.at[0])
    load_rhs = pltpu.make_async_copy(source_hbm.at[0, 0], rhs, load_sem.at[1])
    load_factor = pltpu.make_async_copy(decay_hbm.at[0, 0], factor, load_sem.at[2])
    load_w = [
        pltpu.make_async_copy(w_hbm.at[0, 0, part], w.at[part], w_sem.at[n])
        for n, part in enumerate((upper, lower))
    ]
    load_face.start()
    load_code.start()
    load_u.start()

    barrier = pltpu.get_barrier_semaphore()
    for offset in offsets:
        target = (p - offset + lat_count) % lat_count
        pl.semaphore_signal(barrier, inc=1, device_id={"lat": target}, device_id_type=MESH)

    below, above = (r - 1 + rad_count) % rad_count, (r + 1) % rad_count
    first_layer, last_layer = r == 0, r == rad_count - 1
    inner_layer = jnp.logical_and(r > 0, r < rad_count - 1)

    @pl.when(r > 0)
    def _():
        pl.semaphore_signal(barrier, inc=1, device_id={"rad": below}, device_id_type=MESH)

    @pl.when(r < rad_count - 1)
    def _():
        pl.semaphore_signal(barrier, inc=1, device_id={"rad": above}, device_id_type=MESH)

    load_diag.start()
    for copy in load_w:
        copy.start()
    load_rhs.start()
    load_factor.start()

    inner = (r + rad_count - 1) // rad_count + (2 * rad_count - 2 - r) // rad_count

    def lat_copy(outer, k):
        target = (p - offsets[k] + lat_count) % lat_count
        return pltpu.make_async_remote_copy(
            src_ref=lat_out.at[outer, k], dst_ref=lat_in.at[outer, k],
            send_sem=lat_send.at[outer, k], recv_sem=lat_recv.at[outer, k],
            device_id={"lat": target}, device_id_type=MESH,
        )

    def lat_arrival(outer, k):
        return pltpu.make_async_remote_copy(
            src_ref=lat_out.at[outer, k], dst_ref=lat_in.at[outer, k],
            send_sem=lat_send.at[outer, k], recv_sem=lat_recv.at[outer, k],
            device_id={"lat": (p + 1) % lat_count}, device_id_type=MESH,
        )

    def dn_copy(sweep):
        return pltpu.make_async_remote_copy(
            src_ref=dn_out.at[sweep], dst_ref=dn_in.at[sweep],
            send_sem=dn_send.at[sweep], recv_sem=dn_recv.at[sweep],
            device_id={"rad": below}, device_id_type=MESH,
        )

    def h_copy(sweep, c):
        rows = pl.ds(c * size, size)
        return pltpu.make_async_remote_copy(
            src_ref=h_out.at[sweep, rows], dst_ref=h_in.at[sweep, rows],
            send_sem=h_send.at[sweep, c], recv_sem=h_recv.at[sweep, c],
            device_id={"rad": above}, device_id_type=MESH,
        )

    def make_hot(k):
        target = (p - offsets[k] + lat_count) % lat_count
        hot[k] = one_hot(code_at[k, target], side)

    def make_face(outer, k):
        target = (p - offsets[k] + lat_count) % lat_count
        which = jnp.full((nodes, lanes), face_at[k, target], jnp.int32)
        face = u[slice(0, nodes), :]
        for f in range(1, 4):
            face = jnp.where(which == f, u[slice(f * nodes, (f + 1) * nodes), :], face)
        lat_out[outer, k] = permuted(hot[k], face)

    def product(rows, columns):
        return jnp.dot(w[rows, columns], ub[columns, :], preferred_element_type=jnp.float32)

    def residual(rows):
        return rhs[rows, :] - (acc[rows, :] + diag[rows, :] * u[rows, :])

    def round_u(rows):
        ub[rows, :] = u[rows, :].astype(jnp.bfloat16)

    def send_low(sweep):
        res = residual(bottom)
        dn_out[sweep] = res
        u[bottom, :] = u[bottom, :] + OMEGA * res

        @pl.when(r > 0)
        def _():
            dn_copy(sweep).start()

        res = residual(top)
        res_top[...] = res
        u[top, :] = u[top, :] + OMEGA * res

        @pl.when(first_layer)
        def _():
            h_out[sweep] = factor[...] * res_top[...]
            for c in range(CHUNKS):
                h_copy(sweep, c).start()

    def update_upper():
        u[upper, :] = u[upper, :] + OMEGA * residual(upper)
        round_u(upper)

    def take_h(sweep, relay):
        for c in range(CHUNKS):
            rows = slice(c * size, (c + 1) * size)
            from_bottom = slice(4 * nodes + c * size, 4 * nodes + (c + 1) * size)
            with scope("wh%d" % c):
                h_copy(sweep, c).wait_recv()
            if relay:
                h_out[sweep, rows] = factor[rows, :] * (h_in[sweep, rows] + res_top[rows, :])
                h_copy(sweep, c).start()
            u[from_bottom, :] = u[from_bottom, :] + OMEGA * COUPLE * h_in[sweep, rows]

    def take_dn(sweep):
        with scope("wdn"):
            dn_copy(sweep).wait_recv()
        u[top, :] = u[top, :] + OMEGA * COUPLE * dn_in[sweep]

    def add(rows, columns):
        acc[rows, :] = acc[rows, :] + product(rows, columns)

    def exchange_low(sweep, urgent, then, rest):
        @pl.when(first_layer)
        def _():
            round_u(bottom)
            add(every, bottom)
            take_dn(sweep)
            round_u(top)
            with scope("finish"):
                add(urgent, top)

        @pl.when(last_layer)
        def _():
            round_u(top)
            add(every, top)
            take_h(sweep, False)
            round_u(bottom)
            with scope("finish"):
                add(urgent, bottom)

        @pl.when(inner_layer)
        def _():
            take_h(sweep, True)
            take_dn(sweep)
            round_u(lower)
            with scope("finish"):
                add(urgent, lower)

        then()

        @pl.when(first_layer)
        def _():
            add(rest, top)

        @pl.when(last_layer)
        def _():
            add(rest, bottom)

        @pl.when(inner_layer)
        def _():
            add(rest, lower)

    load_face.wait()
    load_code.wait()
    for k in SEND_ORDER:
        make_hot(k)
    with scope("loadu"):
        load_u.wait()
    with scope("mkf"):
        make_face(0, SEND_ORDER[0])
    with scope("bar"):
        pl.semaphore_wait(barrier, len(offsets) + inner)
    lat_copy(0, SEND_ORDER[0]).start()
    with scope("mkf2"):
        for k in SEND_ORDER[1:]:
            make_face(0, k)
            lat_copy(0, k).start()
    round_u(every)
    load_diag.wait()
    for block in range(6 * nodes // lanes):
        own = slice(block * lanes, (block + 1) * lanes)
        diag[own, :] = jnp.broadcast_to(diag_row[:, own], (lanes, lanes)).T
    with scope("waitw"):
        load_rhs.wait()
        load_factor.wait()
        for copy in load_w:
            copy.wait()
    with scope("acc0"):
        acc[...] = product(every, every)

    near = lax.rem(p, 2)
    for outer in range(ITERS):
        with scope("lres"):
            u[...] = u[...] + OMEGA * residual(every)
            round_u(lower)
        with scope("lacc"):
            acc[...] = product(every, lower)
        arrivals = (1 - near, 2, 3, near)
        for turn, k in enumerate(arrivals):
            own = pl.ds(pl.multiple_of(k * nodes, nodes), nodes)
            with scope("wlat%d" % turn):
                lat_arrival(outer, k).wait_recv()
            with scope("alat%d" % turn):
                u[own, :] = u[own, :] + OMEGA * COUPLE * lat_in[outer, k]
                round_u(own)
                add(every if turn < 3 else lower, own)
        sweep = outer * RADIAL_PASSES
        with scope("sendlow"):
            send_low(sweep)
        with scope("resup"):
            add(upper, pl.ds(pl.multiple_of(near * nodes, nodes), nodes))
            update_upper()
        with scope("accup"):
            acc[...] = product(every, upper)

        if outer < ITERS - 1:

            def then():
                with scope("resup2"):
                    update_upper()
                with scope("mkf3"):
                    for k in SEND_ORDER:
                        make_face(outer + 1, k)
                        lat_copy(outer + 1, k).start()

            exchange_low(sweep, upper, then, lower)
            with scope("sendlow2"):
                send_low(sweep + 1)
            with scope("accup2"):
                acc[...] = product(every, upper)

            @pl.when(first_layer)
            def _():
                round_u(bottom)
                add(every, bottom)
                take_dn(sweep + 1)
                round_u(top)
                add(every, top)

            @pl.when(last_layer)
            def _():
                round_u(top)
                add(every, top)
                take_h(sweep + 1, False)
                round_u(bottom)
                add(every, bottom)

            @pl.when(inner_layer)
            def _():
                take_h(sweep + 1, True)
                take_dn(sweep + 1)
                round_u(lower)
                add(every, lower)
        else:

            def then():
                with scope("sendlow3"):
                    send_low(sweep + 1)

            exchange_low(sweep, lower, then, upper)
            with scope("lastup"):
                u[upper, :] = u[upper, :] + OMEGA * residual(upper)
    final = ITERS * RADIAL_PASSES - 1
    stores = [
        pltpu.make_async_copy(u.at[part], out_hbm.at[0, 0, part], out_sem.at[n])
        for n, part in enumerate((upper, bottom, top))
    ]
    stores[0].start()

    @pl.when(first_layer)
    def _():
        stores[1].start()
        take_dn(final)
        stores[2].start()

    @pl.when(last_layer)
    def _():
        stores[2].start()
        take_h(final, False)
        stores[1].start()

    @pl.when(inner_layer)
    def _():
        take_h(final, True)
        stores[1].start()
        take_dn(final)
        stores[2].start()

    with scope("wsend"):
        for outer in range(ITERS):
            for k in SEND_ORDER:
                lat_copy(outer, k).wait_send()

        @pl.when(r > 0)
        def _():
            for sweep in range(ITERS * RADIAL_PASSES):
                dn_copy(sweep).wait_send()

        @pl.when(r < rad_count - 1)
        def _():
            for sweep in range(ITERS * RADIAL_PASSES):
                for c in range(CHUNKS):
                    h_copy(sweep, c).wait_send()

    with scope("wout"):
        for copy in stores:
            copy.wait()


def per_device(lat_count, rad_count, schur_off, schur_diag, source, start, decay, neighbour_face, orientation):
    order, columns = source.shape[2:]
    nodes = order // 6
    sweeps = ITERS * RADIAL_PASSES
    patches, contacts = neighbour_face.shape
    faces = lambda *lead: pltpu.VMEM((*lead, nodes, columns), jnp.float32)
    wide = lambda dtype: pltpu.VMEM((order, columns), dtype)
    dma = lambda *shape: pltpu.SemaphoreType.DMA(shape)
    hbm = pl.BlockSpec(memory_space=pltpu.HBM)
    return pl.pallas_call(
        functools.partial(kernel, lat_count, rad_count, nodes),
        out_shape=jax.ShapeDtypeStruct(source.shape, jnp.float32),
        in_specs=[hbm] * 7,
        out_specs=pl.BlockSpec(memory_space=pl.ANY),
        scratch_shapes=[
            pltpu.SMEM((contacts, patches), jnp.int32),
            pltpu.SMEM((contacts, patches), jnp.int32),
            pltpu.VMEM((1, order), jnp.float32),
            pltpu.VMEM((order, order), jnp.bfloat16),
            wide(jnp.float32),
            wide(jnp.bfloat16),
            wide(jnp.float32),
            faces(),
            wide(jnp.float32),
            wide(jnp.float32),
            faces(),
            pltpu.VMEM((4, nodes, nodes), jnp.bfloat16),
            faces(ITERS, 4), faces(ITERS, 4), faces(sweeps), faces(sweeps), faces(sweeps), faces(sweeps),
            dma(3), dma(3), dma(2), dma(3),
            dma(ITERS, 4), dma(ITERS, 4), dma(sweeps), dma(sweeps),
            dma(sweeps, CHUNKS), dma(sweeps, CHUNKS),
        ],
        compiler_params=pltpu.CompilerParams(
            collective_id=0, has_side_effects=True, vmem_limit_bytes=24 * 1024 * 1024
        ),
        name="shell",
    )(*(
        pltpu.with_memory_space_constraint(x, pltpu.HBM)
        for x in (neighbour_face.T, orientation.T, schur_diag, schur_off, source, start, decay)
    ))


def solution(mesh):
    lat_count, rad_count = mesh.shape["lat"], mesh.shape["rad"]
    return jax.shard_map(
        functools.partial(per_device, lat_count, rad_count),
        mesh=mesh,
        in_specs=(
            P("lat", "rad", None, None),
            P("lat", "rad", None),
            P("lat", "rad", None, None),
            P("lat", "rad", None, None),
            P("lat", "rad", None, None),
            P(),
            P(),
        ),
        out_specs=P("lat", "rad", None, None),
        check_vma=False,
    )
```

```python
import contextlib
import functools
import math

import jax
import jax.numpy as jnp
from jax import lax
from jax.experimental import pallas as pl
from jax.experimental.pallas import tpu as pltpu
from jax.sharding import PartitionSpec as P

ITERS = 2
RADIAL_PASSES = 2
OMEGA = 0.3
COUPLE = 0.5
CHUNKS = 16
SEND_ORDER = (2, 3, 0, 1)
MESH = pl.DeviceIdType.MESH


def scope(name):
    return contextlib.nullcontext()


def one_hot(code, side):
    nodes = side * side
    n = lax.broadcasted_iota(jnp.int32, (nodes, 1), 0)
    i, j = n // side, n % side
    swap, rows, cols = code & 1, (code >> 1) & 1, (code >> 2) & 1
    a = i + swap * (j - i)
    b = j + swap * (i - j)
    a = a + rows * (side - 1 - 2 * a)
    b = b + cols * (side - 1 - 2 * b)
    at = lax.broadcasted_iota(jnp.int32, (nodes, nodes), 1)
    return jnp.where(at == a * side + b, 1.0, 0.0).astype(jnp.bfloat16)


def permuted(hot, face):
    high = face.astype(jnp.bfloat16)
    rest = face - high.astype(jnp.float32)
    middle = rest.astype(jnp.bfloat16)
    low = (rest - middle.astype(jnp.float32)).astype(jnp.bfloat16)
    total = None
    for part in (low, middle, high):
        moved = jnp.dot(hot, part, preferred_element_type=jnp.float32)
        total = moved if total is None else total + moved
    return total


def kernel(
    lat_count, rad_count, nodes,
    face_hbm, code_hbm, diag_hbm, w_hbm, source_hbm, start_hbm, decay_hbm,
    out_hbm,
    face_at, code_at, diag_row, w, u, ub, rhs, factor, diag, acc, res_top, hot,
    lat_out, lat_in, dn_out, dn_in, h_out, h_in,
    small_sem, load_sem, w_sem, out_sem,
    lat_send, lat_recv, dn_send, dn_recv, h_send, h_recv,
):
    side = math.isqrt(nodes)
    far = max(2, lat_count // 8)
    offsets = (-1, 1, -far, far)
    p = lax.axis_index("lat")
    r = lax.axis_index("rad")
    size = nodes // CHUNKS
    lanes = u.shape[1]
    upper, lower, every = slice(0, 4 * nodes), slice(4 * nodes, 6 * nodes), slice(0, 6 * nodes)
    bottom, top = slice(4 * nodes, 5 * nodes), slice(5 * nodes, 6 * nodes)

    load_face = pltpu.make_async_copy(face_hbm, face_at, small_sem.at[0])
    load_code = pltpu.make_async_copy(code_hbm, code_at, small_sem.at[1])
    load_diag = pltpu.make_async_copy(diag_hbm.at[0], diag_row, small_sem.at[2])
    load_u = pltpu.make_async_copy(start_hbm.at[0, 0], u, load_sem.at[0])
    load_rhs = pltpu.make_async_copy(source_hbm.at[0, 0], rhs, load_sem.at[1])
    load_factor = pltpu.make_async_copy(decay_hbm.at[0, 0], factor, load_sem.at[2])
    load_w = [
        pltpu.make_async_copy(w_hbm.at[0, 0, part], w.at[part], w_sem.at[n])
        for n, part in enumerate((upper, lower))
    ]
    load_face.start()
    load_code.start()
    load_u.start()

    barrier = pltpu.get_barrier_semaphore()
    for offset in offsets:
        target = (p - offset + lat_count) % lat_count
        pl.semaphore_signal(barrier, inc=1, device_id={"lat": target}, device_id_type=MESH)

    below, above = (r - 1 + rad_count) % rad_count, (r + 1) % rad_count
    first_layer, last_layer = r == 0, r == rad_count - 1
    inner_layer = jnp.logical_and(r > 0, r < rad_count - 1)

    @pl.when(r > 0)
    def _():
        pl.semaphore_signal(barrier, inc=1, device_id={"rad": below}, device_id_type=MESH)

    @pl.when(r < rad_count - 1)
    def _():
        pl.semaphore_signal(barrier, inc=1, device_id={"rad": above}, device_id_type=MESH)

    load_diag.start()
    for copy in load_w:
        copy.start()
    load_rhs.start()
    load_factor.start()

    inner = (r + rad_count - 1) // rad_count + (2 * rad_count - 2 - r) // rad_count

    def lat_copy(outer, k):
        target = (p - offsets[k] + lat_count) % lat_count
        return pltpu.make_async_remote_copy(
            src_ref=lat_out.at[outer, k], dst_ref=lat_in.at[outer, k],
            send_sem=lat_send.at[outer], recv_sem=lat_recv.at[outer, k],
            device_id={"lat": target}, device_id_type=MESH,
        )

    def lat_arrival(outer, k):
        return pltpu.make_async_remote_copy(
            src_ref=lat_out.at[outer, k], dst_ref=lat_in.at[outer, k],
            send_sem=lat_send.at[outer], recv_sem=lat_recv.at[outer, k],
            device_id={"lat": (p + 1) % lat_count}, device_id_type=MESH,
        )

    def dn_copy(sweep):
        return pltpu.make_async_remote_copy(
            src_ref=dn_out.at[sweep], dst_ref=dn_in.at[sweep],
            send_sem=dn_send.at[sweep], recv_sem=dn_recv.at[sweep % 2],
            device_id={"rad": below}, device_id_type=MESH,
        )

    def h_copy(sweep, c):
        rows = pl.ds(c * size, size)
        return pltpu.make_async_remote_copy(
            src_ref=h_out.at[sweep, rows], dst_ref=h_in.at[sweep, rows],
            send_sem=h_send.at[sweep], recv_sem=h_recv.at[sweep % 2, c],
            device_id={"rad": above}, device_id_type=MESH,
        )

    def lat_sent(outer):
        return pltpu.make_async_remote_copy(
            src_ref=lat_out.at[outer], dst_ref=lat_in.at[outer],
            send_sem=lat_send.at[outer], recv_sem=lat_recv.at[outer, 0],
            device_id={"lat": (p + 1) % lat_count}, device_id_type=MESH,
        )

    def h_sent(sweep):
        return pltpu.make_async_remote_copy(
            src_ref=h_out.at[sweep], dst_ref=h_in.at[sweep],
            send_sem=h_send.at[sweep], recv_sem=h_recv.at[sweep % 2, 0],
            device_id={"rad": above}, device_id_type=MESH,
        )

    def make_hot(k):
        target = (p - offsets[k] + lat_count) % lat_count
        hot[k] = one_hot(code_at[k, target], side)

    def make_face(outer, k):
        target = (p - offsets[k] + lat_count) % lat_count
        which = jnp.full((nodes, lanes), face_at[k, target], jnp.int32)
        face = u[slice(0, nodes), :]
        for f in range(1, 4):
            face = jnp.where(which == f, u[slice(f * nodes, (f + 1) * nodes), :], face)
        lat_out[outer, k] = permuted(hot[k], face)

    def product(rows, columns):
        return jnp.dot(w[rows, columns], ub[columns, :], preferred_element_type=jnp.float32)

    def residual(rows):
        return rhs[rows, :] - (acc[rows, :] + diag[rows, :] * u[rows, :])

    def round_u(rows):
        ub[rows, :] = u[rows, :].astype(jnp.bfloat16)

    def send_low(sweep):
        res = residual(bottom)
        dn_out[sweep] = res
        u[bottom, :] = u[bottom, :] + OMEGA * res

        @pl.when(r > 0)
        def _():
            dn_copy(sweep).start()

        res = residual(top)
        res_top[...] = res
        u[top, :] = u[top, :] + OMEGA * res

        @pl.when(first_layer)
        def _():
            h_out[sweep] = factor[...] * res_top[...]
            for c in range(CHUNKS):
                h_copy(sweep, c).start()

    def update_upper():
        u[upper, :] = u[upper, :] + OMEGA * residual(upper)
        round_u(upper)

    def take_h(sweep, relay):
        for c in range(CHUNKS):
            rows = slice(c * size, (c + 1) * size)
            from_bottom = slice(4 * nodes + c * size, 4 * nodes + (c + 1) * size)
            with scope("wh%d" % c):
                h_copy(sweep, c).wait_recv()
            if relay:
                h_out[sweep, rows] = factor[rows, :] * (h_in[sweep, rows] + res_top[rows, :])
                h_copy(sweep, c).start()
            u[from_bottom, :] = u[from_bottom, :] + OMEGA * COUPLE * h_in[sweep, rows]

    def take_dn(sweep):
        with scope("wdn"):
            dn_copy(sweep).wait_recv()
        u[top, :] = u[top, :] + OMEGA * COUPLE * dn_in[sweep]

    def blocks(rows):
        return [slice(at, at + nodes) for at in range(rows.start, rows.stop, nodes)]

    def add(rows, columns):
        for block in blocks(rows):
            acc[block, :] = acc[block, :] + product(block, columns)

    def begin(columns):
        for block in blocks(every):
            acc[block, :] = product(block, columns)

    def exchange_low(sweep, urgent, then, rest):
        @pl.when(first_layer)
        def _():
            round_u(bottom)
            add(every, bottom)
            take_dn(sweep)
            round_u(top)
            with scope("finish"):
                add(urgent, top)

        @pl.when(last_layer)
        def _():
            round_u(top)
            add(every, top)
            take_h(sweep, False)
            round_u(bottom)
            with scope("finish"):
                add(urgent, bottom)

        @pl.when(inner_layer)
        def _():
            take_h(sweep, True)
            take_dn(sweep)
            round_u(lower)
            with scope("finish"):
                add(urgent, lower)

        then()

        @pl.when(first_layer)
        def _():
            add(rest, top)

        @pl.when(last_layer)
        def _():
            add(rest, bottom)

        @pl.when(inner_layer)
        def _():
            add(rest, lower)

    load_face.wait()
    load_code.wait()
    for k in SEND_ORDER:
        make_hot(k)
    with scope("loadu"):
        load_u.wait()
    with scope("mkf"):
        make_face(0, SEND_ORDER[0])
    with scope("bar"):
        pl.semaphore_wait(barrier, len(offsets) + inner)
    lat_copy(0, SEND_ORDER[0]).start()
    with scope("mkf2"):
        for k in SEND_ORDER[1:]:
            make_face(0, k)
            lat_copy(0, k).start()
    round_u(every)
    load_diag.wait()
    for block in range(6 * nodes // lanes):
        own = slice(block * lanes, (block + 1) * lanes)
        diag[own, :] = jnp.broadcast_to(diag_row[:, own], (lanes, lanes)).T
    with scope("waitw"):
        load_rhs.wait()
        load_factor.wait()
        for copy in load_w:
            copy.wait()
    with scope("acc0"):
        begin(every)

    near = lax.rem(p, 2)
    for outer in range(ITERS):
        with scope("lres"):
            u[...] = u[...] + OMEGA * residual(every)
            round_u(lower)
        with scope("lacc"):
            begin(lower)
        arrivals = (1 - near, 2, 3, near)
        for turn, k in enumerate(arrivals):
            own = pl.ds(pl.multiple_of(k * nodes, nodes), nodes)
            with scope("wlat%d" % turn):
                lat_arrival(outer, k).wait_recv()
            with scope("alat%d" % turn):
                u[own, :] = u[own, :] + OMEGA * COUPLE * lat_in[outer, k]
                round_u(own)
                add(every if turn < 3 else lower, own)
        sweep = outer * RADIAL_PASSES
        with scope("sendlow"):
            send_low(sweep)
        with scope("resup"):
            add(upper, pl.ds(pl.multiple_of(near * nodes, nodes), nodes))
            update_upper()
        with scope("accup"):
            begin(upper)

        if outer < ITERS - 1:

            def then():
                with scope("resup2"):
                    update_upper()
                with scope("mkf3"):
                    for k in SEND_ORDER:
                        make_face(outer + 1, k)
                        lat_copy(outer + 1, k).start()

            exchange_low(sweep, upper, then, lower)
            with scope("sendlow2"):
                send_low(sweep + 1)
            with scope("accup2"):
                begin(upper)

            @pl.when(first_layer)
            def _():
                round_u(bottom)
                add(every, bottom)
                take_dn(sweep + 1)
                round_u(top)
                add(every, top)

            @pl.when(last_layer)
            def _():
                round_u(top)
                add(every, top)
                take_h(sweep + 1, False)
                round_u(bottom)
                add(every, bottom)

            @pl.when(inner_layer)
            def _():
                take_h(sweep + 1, True)
                take_dn(sweep + 1)
                round_u(lower)
                add(every, lower)
        else:

            def then():
                with scope("sendlow3"):
                    send_low(sweep + 1)

            exchange_low(sweep, lower, then, upper)
            with scope("lastup"):
                u[upper, :] = u[upper, :] + OMEGA * residual(upper)
    final = ITERS * RADIAL_PASSES - 1
    stores = [
        pltpu.make_async_copy(u.at[part], out_hbm.at[0, 0, part], out_sem.at[n])
        for n, part in enumerate((upper, bottom, top))
    ]
    stores[0].start()

    @pl.when(first_layer)
    def _():
        stores[1].start()
        take_dn(final)
        stores[2].start()

    @pl.when(last_layer)
    def _():
        stores[2].start()
        take_h(final, False)
        stores[1].start()

    @pl.when(inner_layer)
    def _():
        take_h(final, True)
        stores[1].start()
        take_dn(final)
        stores[2].start()

    with scope("wsend"):
        for outer in range(ITERS):
            lat_sent(outer).wait_send()

        @pl.when(r > 0)
        def _():
            for sweep in range(ITERS * RADIAL_PASSES):
                dn_copy(sweep).wait_send()

        @pl.when(r < rad_count - 1)
        def _():
            for sweep in range(ITERS * RADIAL_PASSES):
                h_sent(sweep).wait_send()

    with scope("wout"):
        for copy in stores:
            copy.wait()


def per_device(lat_count, rad_count, schur_off, schur_diag, source, start, decay, neighbour_face, orientation):
    order, columns = source.shape[2:]
    nodes = order // 6
    sweeps = ITERS * RADIAL_PASSES
    patches, contacts = neighbour_face.shape
    faces = lambda *lead: pltpu.VMEM((*lead, nodes, columns), jnp.float32)
    wide = lambda dtype: pltpu.VMEM((order, columns), dtype)
    dma = lambda *shape: pltpu.SemaphoreType.DMA(shape)
    hbm = pl.BlockSpec(memory_space=pltpu.HBM)
    return pl.pallas_call(
        functools.partial(kernel, lat_count, rad_count, nodes),
        out_shape=jax.ShapeDtypeStruct(source.shape, jnp.float32),
        in_specs=[hbm] * 7,
        out_specs=pl.BlockSpec(memory_space=pl.ANY),
        scratch_shapes=[
            pltpu.SMEM((contacts, patches), jnp.int32),
            pltpu.SMEM((contacts, patches), jnp.int32),
            pltpu.VMEM((1, order), jnp.float32),
            pltpu.VMEM((order, order), jnp.bfloat16),
            wide(jnp.float32),
            wide(jnp.bfloat16),
            wide(jnp.float32),
            faces(),
            wide(jnp.float32),
            wide(jnp.float32),
            faces(),
            pltpu.VMEM((4, nodes, nodes), jnp.bfloat16),
            faces(ITERS, 4), faces(ITERS, 4), faces(sweeps), faces(sweeps), faces(sweeps), faces(sweeps),
            dma(3), dma(3), dma(2), dma(3),
            dma(ITERS), dma(ITERS, 4), dma(sweeps), dma(2),
            dma(sweeps), dma(2, CHUNKS),
        ],
        compiler_params=pltpu.CompilerParams(
            collective_id=0, has_side_effects=True, vmem_limit_bytes=24 * 1024 * 1024
        ),
        name="shell",
    )(*(
        pltpu.with_memory_space_constraint(x, pltpu.HBM)
        for x in (neighbour_face.T, orientation.T, schur_diag, schur_off, source, start, decay)
    ))


def solution(mesh):
    lat_count, rad_count = mesh.shape["lat"], mesh.shape["rad"]
    return jax.shard_map(
        functools.partial(per_device, lat_count, rad_count),
        mesh=mesh,
        in_specs=(
            P("lat", "rad", None, None),
            P("lat", "rad", None),
            P("lat", "rad", None, None),
            P("lat", "rad", None, None),
            P("lat", "rad", None, None),
            P(),
            P(),
        ),
        out_specs=P("lat", "rad", None, None),
        check_vma=False,
    )
```

```python
import contextlib
import functools
import math

import jax
import jax.numpy as jnp
from jax import lax
from jax.experimental import pallas as pl
from jax.experimental.pallas import tpu as pltpu
from jax.sharding import PartitionSpec as P

ITERS = 2
RADIAL_PASSES = 2
OMEGA = 0.3
COUPLE = 0.5
CHUNKS = 8
HALVES = (0, 1)
SEND_ORDER = (2, 3, 0, 1)
MESH = pl.DeviceIdType.MESH


def scope(name):
    return contextlib.nullcontext()


def one_hot(code, side):
    nodes = side * side
    n = lax.broadcasted_iota(jnp.int32, (nodes, 1), 0)
    i, j = n // side, n % side
    swap, rows, cols = code & 1, (code >> 1) & 1, (code >> 2) & 1
    a = i + swap * (j - i)
    b = j + swap * (i - j)
    a = a + rows * (side - 1 - 2 * a)
    b = b + cols * (side - 1 - 2 * b)
    at = lax.broadcasted_iota(jnp.int32, (nodes, nodes), 1)
    return jnp.where(at == a * side + b, 1.0, 0.0).astype(jnp.bfloat16)


def permuted(hot, face):
    high = face.astype(jnp.bfloat16)
    rest = face - high.astype(jnp.float32)
    middle = rest.astype(jnp.bfloat16)
    low = (rest - middle.astype(jnp.float32)).astype(jnp.bfloat16)
    total = None
    for part in (low, middle, high):
        moved = jnp.dot(hot, part, preferred_element_type=jnp.float32)
        total = moved if total is None else total + moved
    return total


def kernel(
    lat_count, rad_count, nodes,
    face_hbm, code_hbm, diag_hbm, w_hbm, source_hbm, start_hbm, decay_hbm,
    out_hbm,
    face_at, code_at, diag_row, w, u, ub, rhs, factor, diag, acc, acc_low, packed_factor, packed_top, hot,
    lat_out, lat_in, dn_out, dn_in, h_out, h_in,
    small_sem, load_sem, w_sem, out_sem,
    lat_send, lat_recv, dn_send, dn_recv, h_send, h_recv,
):
    side = math.isqrt(nodes)
    far = max(2, lat_count // 8)
    offsets = (-1, 1, -far, far)
    p = lax.axis_index("lat")
    r = lax.axis_index("rad")
    lanes = u.shape[1]
    half = lanes // 2
    size = nodes // 2 // CHUNKS
    upper, lower, every = slice(0, 4 * nodes), slice(4 * nodes, 6 * nodes), slice(0, 6 * nodes)
    bottom, top = slice(4 * nodes, 5 * nodes), slice(5 * nodes, 6 * nodes)

    load_face = pltpu.make_async_copy(face_hbm, face_at, small_sem.at[0])
    load_code = pltpu.make_async_copy(code_hbm, code_at, small_sem.at[1])
    load_diag = pltpu.make_async_copy(diag_hbm.at[0], diag_row, small_sem.at[2])
    load_u = pltpu.make_async_copy(start_hbm.at[0, 0], u, load_sem.at[0])
    load_rhs = pltpu.make_async_copy(source_hbm.at[0, 0], rhs, load_sem.at[1])
    load_factor = pltpu.make_async_copy(decay_hbm.at[0, 0], factor, load_sem.at[2])
    load_w = [
        pltpu.make_async_copy(w_hbm.at[0, 0, part], w.at[part], w_sem.at[n])
        for n, part in enumerate((upper, lower))
    ]
    load_face.start()
    load_code.start()
    load_u.start()

    barrier = pltpu.get_barrier_semaphore()
    for offset in offsets:
        target = (p - offset + lat_count) % lat_count
        pl.semaphore_signal(barrier, inc=1, device_id={"lat": target}, device_id_type=MESH)

    below, above = (r - 1 + rad_count) % rad_count, (r + 1) % rad_count
    first_layer, last_layer = r == 0, r == rad_count - 1
    inner_layer = jnp.logical_and(r > 0, r < rad_count - 1)
    second_layer = jnp.logical_and(r == 1, r < rad_count - 1)
    later_layer = jnp.logical_and(r > 1, r < rad_count - 1)

    @pl.when(r > 0)
    def _():
        pl.semaphore_signal(barrier, inc=1, device_id={"rad": below}, device_id_type=MESH)

    @pl.when(r < rad_count - 1)
    def _():
        pl.semaphore_signal(barrier, inc=1, device_id={"rad": above}, device_id_type=MESH)

    load_diag.start()
    for copy in load_w:
        copy.start()
    load_rhs.start()
    load_factor.start()

    inner = (r + rad_count - 1) // rad_count + (2 * rad_count - 2 - r) // rad_count

    def in_half(s, rows):
        lane = lax.broadcasted_iota(jnp.int32, (rows, lanes), 1)
        return lane < half if s == 0 else lane >= half

    def pack(x, s):
        first, second = x[: nodes // 2, :], x[nodes // 2 :, :]
        left = in_half(0, nodes // 2)
        if s == 0:
            return jnp.where(left, first, pltpu.roll(second, half, 1))
        return jnp.where(left, pltpu.roll(first, half, 1), second)

    def unpack(x, s):
        moved = pltpu.roll(x, half, 1)
        return jnp.concatenate([x, moved] if s == 0 else [moved, x], axis=0)

    def gain(rows, value, s):
        u[rows, :] = u[rows, :] + jnp.where(in_half(s, value.shape[0]), value, 0.0)

    def lat_copy(outer, s, k, target):
        return pltpu.make_async_remote_copy(
            src_ref=lat_out.at[outer, s, k], dst_ref=lat_in.at[outer, s, k],
            send_sem=lat_send.at[outer], recv_sem=lat_recv.at[outer, s, k],
            device_id={"lat": target}, device_id_type=MESH,
        )

    def lat_target(k):
        return (p - offsets[k] + lat_count) % lat_count

    def lat_sent(outer):
        return pltpu.make_async_remote_copy(
            src_ref=lat_out.at[outer], dst_ref=lat_in.at[outer],
            send_sem=lat_send.at[outer], recv_sem=lat_recv.at[outer, 0, 0],
            device_id={"lat": (p + 1) % lat_count}, device_id_type=MESH,
        )

    def dn_copy(sweep, s):
        return pltpu.make_async_remote_copy(
            src_ref=dn_out.at[sweep, s], dst_ref=dn_in.at[sweep, s],
            send_sem=dn_send.at[sweep], recv_sem=dn_recv.at[sweep % 2, s],
            device_id={"rad": below}, device_id_type=MESH,
        )

    def dn_sent(sweep):
        return pltpu.make_async_remote_copy(
            src_ref=dn_out.at[sweep], dst_ref=dn_in.at[sweep],
            send_sem=dn_send.at[sweep], recv_sem=dn_recv.at[sweep % 2, 0],
            device_id={"rad": below}, device_id_type=MESH,
        )

    def h_copy(sweep, s, c):
        rows = pl.ds(c * size, size)
        return pltpu.make_async_remote_copy(
            src_ref=h_out.at[sweep, s, rows], dst_ref=h_in.at[sweep, s, rows],
            send_sem=h_send.at[sweep], recv_sem=h_recv.at[sweep % 2, s, c],
            device_id={"rad": above}, device_id_type=MESH,
        )

    def h_sent(sweep):
        return pltpu.make_async_remote_copy(
            src_ref=h_out.at[sweep], dst_ref=h_in.at[sweep],
            send_sem=h_send.at[sweep], recv_sem=h_recv.at[sweep % 2, 0, 0],
            device_id={"rad": above}, device_id_type=MESH,
        )

    def make_hot(k):
        hot[k] = one_hot(code_at[k, lat_target(k)], side)

    def oriented(k):
        which = jnp.full((nodes, lanes), face_at[k, lat_target(k)], jnp.int32)
        face = u[slice(0, nodes), :]
        for f in range(1, 4):
            face = jnp.where(which == f, u[slice(f * nodes, (f + 1) * nodes), :], face)
        return permuted(hot[k], face)

    def send_faces(outer, s):
        for pair in (SEND_ORDER[:2], SEND_ORDER[2:]):
            faces = [pack(oriented(k), s) for k in pair]
            for k, face in zip(pair, faces):
                lat_out[outer, s, k] = face
            for k in pair:
                lat_copy(outer, s, k, lat_target(k)).start()

    def product(rows, columns):
        return jnp.dot(w[rows, columns], ub[columns, :], preferred_element_type=jnp.float32)

    def blocks(rows):
        return [slice(at, at + nodes) for at in range(rows.start, rows.stop, nodes)]

    def add(rows, columns):
        for block in blocks(rows):
            acc[block, :] = acc[block, :] + product(block, columns)

    def begin(columns):
        for block in blocks(every):
            acc[block, :] = product(block, columns)

    def left_over(rows, total):
        return rhs[rows, :] - (total + diag[rows, :] * u[rows, :])

    def residual(rows):
        return left_over(rows, acc[rows, :])

    def round_u(rows):
        ub[rows, :] = u[rows, :].astype(jnp.bfloat16)

    def round_half(rows, s):
        count = rows.stop - rows.start
        old = ub[rows, :].astype(jnp.float32)
        ub[rows, :] = jnp.where(in_half(s, count), u[rows, :], old).astype(jnp.bfloat16)

    def send_low(sweep, s, total):
        res = left_over(bottom, total(bottom))
        dn_out[sweep, s] = pack(res, s)

        @pl.when(r > 0)
        def _():
            dn_copy(sweep, s).start()

        gain(bottom, OMEGA * res, s)
        res = left_over(top, total(top))
        packed_top[s] = pack(res, s)

        @pl.when(first_layer)
        def _():
            h_out[sweep, s] = packed_factor[s] * packed_top[s]
            for c in range(CHUNKS):
                h_copy(sweep, s, c).start()

        gain(top, OMEGA * res, s)

    def relay(where, sweep, s):
        @pl.when(where)
        def _():
            with scope("relay%d%d" % (sweep, s)):
                for c in range(CHUNKS):
                    rows = slice(c * size, (c + 1) * size)
                    h_copy(sweep, s, c).wait_recv()
                    h_out[sweep, s, rows] = packed_factor[s, rows] * (
                        h_in[sweep, s, rows] + packed_top[s, rows]
                    )
                    h_copy(sweep, s, c).start()

    def take(sweep, s):
        @pl.when(last_layer)
        def _():
            with scope("take%d%d" % (sweep, s)):
                for c in range(CHUNKS):
                    h_copy(sweep, s, c).wait_recv()

    def apply_h(sweep, s):
        @pl.when(r > 0)
        def _():
            gain(bottom, OMEGA * COUPLE * unpack(h_in[sweep, s], s), s)

    def apply_dn(sweep, s):
        @pl.when(r < rad_count - 1)
        def _():
            with scope("wdn%d%d" % (sweep, s)):
                dn_copy(sweep, s).wait_recv()
            gain(top, OMEGA * COUPLE * unpack(dn_in[sweep, s], s), s)

    def added(rows):
        return acc[rows, :] + product(rows, lower)

    load_face.wait()
    load_code.wait()
    for k in SEND_ORDER:
        make_hot(k)
    with scope("loadu"):
        load_u.wait()
    with scope("mkf"):
        for k in SEND_ORDER:
            face = oriented(k)
            for s in HALVES:
                lat_out[0, s, k] = pack(face, s)
            if k == SEND_ORDER[0]:
                with scope("bar"):
                    pl.semaphore_wait(barrier, len(offsets) + inner)
            lat_copy(0, 0, k, lat_target(k)).start()
        for k in SEND_ORDER:
            lat_copy(0, 1, k, lat_target(k)).start()
    round_u(every)
    load_diag.wait()
    for block in range(6 * nodes // lanes):
        own = slice(block * lanes, (block + 1) * lanes)
        diag[own, :] = jnp.broadcast_to(diag_row[:, own], (lanes, lanes)).T
    with scope("waitw"):
        load_rhs.wait()
        load_factor.wait()
        for copy in load_w:
            copy.wait()
    for s in HALVES:
        packed_factor[s] = pack(factor[...], s)
    with scope("acc0"):
        begin(every)

    near = lax.rem(p, 2)
    for outer in range(ITERS):
        first, second = outer * RADIAL_PASSES, outer * RADIAL_PASSES + 1
        with scope("lres"):
            u[...] = u[...] + OMEGA * residual(every)
            round_u(lower)
        with scope("lacc"):
            begin(lower)
            acc_low[...] = acc[lower, :]
        for s in HALVES:
            total = acc_low if s == 0 else acc.at[lower]
            for turn, k in enumerate((1 - near, 2, 3, near)):
                own = pl.ds(pl.multiple_of(k * nodes, nodes), nodes)
                with scope("wlat%d%d" % (s, turn)):
                    lat_copy(outer, s, k, (p + 1) % lat_count).wait_recv()
                gain(own, OMEGA * COUPLE * unpack(lat_in[outer, s, k], s), s)
                round_u(own)
                columns = own
                if outer == 1:
                    if turn < 3:
                        continue
                    columns = upper
                for block in (slice(0, nodes), slice(nodes, 2 * nodes)):
                    rows = slice(4 * nodes + block.start, 4 * nodes + block.stop)
                    total[block, :] = total[block, :] + product(rows, columns)
                if outer == 0 and s == 1 and turn == 0:
                    relay(second_layer, first, 0)
            with scope("sendlow%d" % s):
                if s == 0:
                    send_low(first, s, lambda rows: acc_low[rows.start - 4 * nodes : rows.stop - 4 * nodes, :])
                else:
                    send_low(first, s, lambda rows: acc[rows, :])
        if outer == 0:
            relay(later_layer, first, 0)
        with scope("bulk1"):
            add(upper, upper)
            u[upper, :] = u[upper, :] + OMEGA * residual(upper)
            round_u(upper)
        if outer == 1:
            relay(second_layer, first, 0)
        with scope("bulk2"):
            begin(upper)
        relay(second_layer, first, 1)
        if outer == 1:
            relay(later_layer, first, 0)
            relay(later_layer, first, 1)
        for s in HALVES:
            take(first, s)
            apply_h(first, s)
            apply_dn(first, s)
            with scope("fin%d" % s):
                round_half(lower, s)
                if outer < ITERS - 1:
                    for block in blocks(upper):
                        gain(block, OMEGA * left_over(block, added(block)), s)
            with scope("sendlow2%d" % s):
                sums = added(lower)
                send_low(second, s, lambda rows: sums[rows.start - 4 * nodes : rows.stop - 4 * nodes, :])
            if outer < ITERS - 1:
                if s == 0:
                    relay(later_layer, first, 1)
                else:
                    relay(second_layer, second, 0)
                with scope("faces%d" % s):
                    send_faces(outer + 1, s)
        if outer < ITERS - 1:
            relay(later_layer, second, 0)
            relay(inner_layer, second, 1)
            with scope("bulk3"):
                round_u(upper)
                begin(upper)
            for s in HALVES:
                take(second, s)
                apply_h(second, s)
                apply_dn(second, s)
            with scope("bulk4"):
                round_u(lower)
                add(every, lower)
    with scope("lastup"):
        for block in blocks(upper):
            u[block, :] = u[block, :] + OMEGA * left_over(block, added(block))
    final = ITERS * RADIAL_PASSES - 1
    stores = [
        pltpu.make_async_copy(u.at[part], out_hbm.at[0, 0, part], out_sem.at[n])
        for n, part in enumerate((upper, bottom, top))
    ]
    stores[0].start()
    for s in HALVES:
        relay(inner_layer, final, s)
        take(final, s)
        apply_h(final, s)
    stores[1].start()
    for s in HALVES:
        apply_dn(final, s)
    stores[2].start()

    with scope("wsend"):
        for outer in range(ITERS):
            lat_sent(outer).wait_send()

        @pl.when(r > 0)
        def _():
            for sweep in range(ITERS * RADIAL_PASSES):
                dn_sent(sweep).wait_send()

        @pl.when(r < rad_count - 1)
        def _():
            for sweep in range(ITERS * RADIAL_PASSES):
                h_sent(sweep).wait_send()

    with scope("wout"):
        for copy in stores:
            copy.wait()


def per_device(lat_count, rad_count, schur_off, schur_diag, source, start, decay, neighbour_face, orientation):
    order, columns = source.shape[2:]
    nodes = order // 6
    sweeps = ITERS * RADIAL_PASSES
    patches, contacts = neighbour_face.shape
    faces = lambda *lead: pltpu.VMEM((*lead, nodes, columns), jnp.float32)
    packed = lambda *lead: pltpu.VMEM((*lead, 2, nodes // 2, columns), jnp.float32)
    wide = lambda dtype: pltpu.VMEM((order, columns), dtype)
    dma = lambda *shape: pltpu.SemaphoreType.DMA(shape)
    hbm = pl.BlockSpec(memory_space=pltpu.HBM)
    return pl.pallas_call(
        functools.partial(kernel, lat_count, rad_count, nodes),
        out_shape=jax.ShapeDtypeStruct(source.shape, jnp.float32),
        in_specs=[hbm] * 7,
        out_specs=pl.BlockSpec(memory_space=pl.ANY),
        scratch_shapes=[
            pltpu.SMEM((contacts, patches), jnp.int32),
            pltpu.SMEM((contacts, patches), jnp.int32),
            pltpu.VMEM((1, order), jnp.float32),
            pltpu.VMEM((order, order), jnp.bfloat16),
            wide(jnp.float32),
            wide(jnp.bfloat16),
            wide(jnp.float32),
            faces(),
            wide(jnp.float32),
            wide(jnp.float32),
            pltpu.VMEM((2 * nodes, columns), jnp.float32),
            packed(),
            packed(),
            pltpu.VMEM((4, nodes, nodes), jnp.bfloat16),
            pltpu.VMEM((ITERS, 2, 4, nodes // 2, columns), jnp.float32),
            pltpu.VMEM((ITERS, 2, 4, nodes // 2, columns), jnp.float32),
            packed(sweeps), packed(sweeps), packed(sweeps), packed(sweeps),
            dma(3), dma(3), dma(2), dma(3),
            dma(ITERS), dma(ITERS, 2, 4), dma(sweeps), dma(2, 2),
            dma(sweeps), dma(2, 2, CHUNKS),
        ],
        compiler_params=pltpu.CompilerParams(
            collective_id=0, has_side_effects=True, vmem_limit_bytes=24 * 1024 * 1024
        ),
        name="shell",
    )(*(
        pltpu.with_memory_space_constraint(x, pltpu.HBM)
        for x in (neighbour_face.T, orientation.T, schur_diag, schur_off, source, start, decay)
    ))


def solution(mesh):
    lat_count, rad_count = mesh.shape["lat"], mesh.shape["rad"]
    return jax.shard_map(
        functools.partial(per_device, lat_count, rad_count),
        mesh=mesh,
        in_specs=(
            P("lat", "rad", None, None),
            P("lat", "rad", None),
            P("lat", "rad", None, None),
            P("lat", "rad", None, None),
            P("lat", "rad", None, None),
            P(),
            P(),
        ),
        out_specs=P("lat", "rad", None, None),
        check_vma=False,
    )
```

```python
import contextlib
import functools
import math

import jax
import jax.numpy as jnp
from jax import lax
from jax.experimental import pallas as pl
from jax.experimental.pallas import tpu as pltpu
from jax.sharding import PartitionSpec as P

ITERS = 2
RADIAL_PASSES = 2
OMEGA = 0.3
COUPLE = 0.5
CHUNKS = 8
HALVES = (0, 1)
SEND_ORDER = (2, 3, 0, 1)
MESH = pl.DeviceIdType.MESH


def scope(name):
    return contextlib.nullcontext()


def one_hot(code, side):
    nodes = side * side
    n = lax.broadcasted_iota(jnp.int32, (nodes, 1), 0)
    i, j = n // side, n % side
    swap, rows, cols = code & 1, (code >> 1) & 1, (code >> 2) & 1
    a = i + swap * (j - i)
    b = j + swap * (i - j)
    a = a + rows * (side - 1 - 2 * a)
    b = b + cols * (side - 1 - 2 * b)
    at = lax.broadcasted_iota(jnp.int32, (nodes, nodes), 1)
    return jnp.where(at == a * side + b, 1.0, 0.0).astype(jnp.bfloat16)


def permuted(hot, face):
    high = face.astype(jnp.bfloat16)
    rest = face - high.astype(jnp.float32)
    middle = rest.astype(jnp.bfloat16)
    low = (rest - middle.astype(jnp.float32)).astype(jnp.bfloat16)
    total = None
    for part in (low, middle, high):
        moved = jnp.dot(hot, part, preferred_element_type=jnp.float32)
        total = moved if total is None else total + moved
    return total


def kernel(
    lat_count, rad_count, nodes,
    face_hbm, code_hbm, diag_hbm, w_hbm, source_hbm, start_hbm, decay_hbm,
    out_hbm,
    face_at, code_at, diag_row, w, u, ub, rhs, factor, diag, sums, packed_factor, packed_top, hot,
    lat_out, lat_in, dn_out, dn_in, h_out, h_in,
    small_sem, load_sem, w_sem, out_sem,
    lat_send, lat_recv, dn_send, dn_recv, h_send, h_recv,
):
    side = math.isqrt(nodes)
    far = max(2, lat_count // 8)
    offsets = (-1, 1, -far, far)
    p = lax.axis_index("lat")
    r = lax.axis_index("rad")
    lanes = u.shape[1]
    half = lanes // 2
    size = nodes // 2 // CHUNKS
    upper, lower, every = slice(0, 4 * nodes), slice(4 * nodes, 6 * nodes), slice(0, 6 * nodes)
    bottom, top = slice(4 * nodes, 5 * nodes), slice(5 * nodes, 6 * nodes)

    load_face = pltpu.make_async_copy(face_hbm, face_at, small_sem.at[0])
    load_code = pltpu.make_async_copy(code_hbm, code_at, small_sem.at[1])
    load_diag = pltpu.make_async_copy(diag_hbm.at[0], diag_row, small_sem.at[2])
    load_u = pltpu.make_async_copy(start_hbm.at[0, 0], u, load_sem.at[0])
    load_rhs = pltpu.make_async_copy(source_hbm.at[0, 0], rhs, load_sem.at[1])
    load_factor = pltpu.make_async_copy(decay_hbm.at[0, 0], factor, load_sem.at[2])
    load_w = [
        pltpu.make_async_copy(w_hbm.at[0, 0, part], w.at[part], w_sem.at[n])
        for n, part in enumerate((upper, lower))
    ]
    load_face.start()
    load_code.start()
    load_u.start()

    barrier = pltpu.get_barrier_semaphore()
    for offset in offsets:
        target = (p - offset + lat_count) % lat_count
        pl.semaphore_signal(barrier, inc=1, device_id={"lat": target}, device_id_type=MESH)

    below, above = (r - 1 + rad_count) % rad_count, (r + 1) % rad_count
    first_layer, last_layer = r == 0, r == rad_count - 1
    inner_layer = jnp.logical_and(r > 0, r < rad_count - 1)
    second_layer = jnp.logical_and(r == 1, r < rad_count - 1)
    later_layer = jnp.logical_and(r > 1, r < rad_count - 1)

    @pl.when(r > 0)
    def _():
        pl.semaphore_signal(barrier, inc=1, device_id={"rad": below}, device_id_type=MESH)

    @pl.when(r < rad_count - 1)
    def _():
        pl.semaphore_signal(barrier, inc=1, device_id={"rad": above}, device_id_type=MESH)

    load_diag.start()
    for copy in load_w:
        copy.start()
    load_rhs.start()
    load_factor.start()

    inner = (r + rad_count - 1) // rad_count + (2 * rad_count - 2 - r) // rad_count

    def in_half(s, rows):
        lane = lax.broadcasted_iota(jnp.int32, (rows, lanes), 1)
        return lane < half if s == 0 else lane >= half

    def pack(x, s):
        first, second = x[: nodes // 2, :], x[nodes // 2 :, :]
        left = in_half(0, nodes // 2)
        if s == 0:
            return jnp.where(left, first, pltpu.roll(second, half, 1))
        return jnp.where(left, pltpu.roll(first, half, 1), second)

    def unpack(x, s):
        moved = pltpu.roll(x, half, 1)
        return jnp.concatenate([x, moved] if s == 0 else [moved, x], axis=0)

    def gain(rows, value, s):
        u[rows, :] = u[rows, :] + jnp.where(in_half(s, value.shape[0]), value, 0.0)

    def lat_copy(outer, s, k, target):
        return pltpu.make_async_remote_copy(
            src_ref=lat_out.at[outer, s, k], dst_ref=lat_in.at[outer, s, k],
            send_sem=lat_send.at[outer], recv_sem=lat_recv.at[outer, s, k],
            device_id={"lat": target}, device_id_type=MESH,
        )

    def lat_target(k):
        return (p - offsets[k] + lat_count) % lat_count

    def lat_sent(outer):
        return pltpu.make_async_remote_copy(
            src_ref=lat_out.at[outer], dst_ref=lat_in.at[outer],
            send_sem=lat_send.at[outer], recv_sem=lat_recv.at[outer, 0, 0],
            device_id={"lat": (p + 1) % lat_count}, device_id_type=MESH,
        )

    def dn_copy(sweep, s):
        return pltpu.make_async_remote_copy(
            src_ref=dn_out.at[sweep, s], dst_ref=dn_in.at[sweep, s],
            send_sem=dn_send.at[sweep], recv_sem=dn_recv.at[sweep % 2, s],
            device_id={"rad": below}, device_id_type=MESH,
        )

    def dn_sent(sweep):
        return pltpu.make_async_remote_copy(
            src_ref=dn_out.at[sweep], dst_ref=dn_in.at[sweep],
            send_sem=dn_send.at[sweep], recv_sem=dn_recv.at[sweep % 2, 0],
            device_id={"rad": below}, device_id_type=MESH,
        )

    def h_copy(sweep, s, c):
        rows = pl.ds(c * size, size)
        return pltpu.make_async_remote_copy(
            src_ref=h_out.at[sweep, s, rows], dst_ref=h_in.at[sweep, s, rows],
            send_sem=h_send.at[sweep], recv_sem=h_recv.at[sweep % 2, s, c],
            device_id={"rad": above}, device_id_type=MESH,
        )

    def h_sent(sweep):
        return pltpu.make_async_remote_copy(
            src_ref=h_out.at[sweep], dst_ref=h_in.at[sweep],
            send_sem=h_send.at[sweep], recv_sem=h_recv.at[sweep % 2, 0, 0],
            device_id={"rad": above}, device_id_type=MESH,
        )

    def make_hot(k):
        hot[k] = one_hot(code_at[k, lat_target(k)], side)

    def oriented(k):
        which = jnp.full((nodes, lanes), face_at[k, lat_target(k)], jnp.int32)
        face = u[slice(0, nodes), :]
        for f in range(1, 4):
            face = jnp.where(which == f, u[slice(f * nodes, (f + 1) * nodes), :], face)
        return permuted(hot[k], face)

    def send_faces(outer, s):
        for pair in (SEND_ORDER[:2], SEND_ORDER[2:]):
            faces = [pack(oriented(k), s) for k in pair]
            for k, face in zip(pair, faces):
                lat_out[outer, s, k] = face
            for k in pair:
                lat_copy(outer, s, k, lat_target(k)).start()

    def product(rows, columns):
        return jnp.dot(w[rows, columns], ub[columns, :], preferred_element_type=jnp.float32)

    def blocks(rows):
        return [slice(at, at + nodes) for at in range(rows.start, rows.stop, nodes)]

    def add(acc, rows, columns):
        for block in blocks(rows):
            acc[block, :] = acc[block, :] + product(block, columns)

    def begin(acc, rows, columns):
        for block in blocks(rows):
            acc[block, :] = product(block, columns)

    def left_over(rows, total):
        return rhs[rows, :] - (total + diag[rows, :] * u[rows, :])

    def round_u(rows):
        ub[rows, :] = u[rows, :].astype(jnp.bfloat16)

    def round_half(rows, s):
        count = rows.stop - rows.start
        old = ub[rows, :].astype(jnp.float32)
        ub[rows, :] = jnp.where(in_half(s, count), u[rows, :], old).astype(jnp.bfloat16)

    def send_low(sweep, s, total):
        res = left_over(bottom, total(bottom))
        dn_out[sweep, s] = pack(res, s)

        @pl.when(r > 0)
        def _():
            dn_copy(sweep, s).start()

        gain(bottom, OMEGA * res, s)
        res = left_over(top, total(top))
        packed_top[s] = pack(res, s)

        @pl.when(first_layer)
        def _():
            h_out[sweep, s] = packed_factor[s] * packed_top[s]
            for c in range(CHUNKS):
                h_copy(sweep, s, c).start()

        gain(top, OMEGA * res, s)

    def relay(where, sweep, s):
        @pl.when(where)
        def _():
            with scope("relay%d%d" % (sweep, s)):
                for c in range(CHUNKS):
                    rows = slice(c * size, (c + 1) * size)
                    h_copy(sweep, s, c).wait_recv()
                    h_out[sweep, s, rows] = packed_factor[s, rows] * (
                        h_in[sweep, s, rows] + packed_top[s, rows]
                    )
                    h_copy(sweep, s, c).start()

    def take(sweep, s):
        @pl.when(last_layer)
        def _():
            with scope("take%d%d" % (sweep, s)):
                for c in range(CHUNKS):
                    h_copy(sweep, s, c).wait_recv()

    def apply_h(sweep, s):
        @pl.when(r > 0)
        def _():
            gain(bottom, OMEGA * COUPLE * unpack(h_in[sweep, s], s), s)

    def apply_dn(sweep, s):
        @pl.when(r < rad_count - 1)
        def _():
            with scope("wdn%d%d" % (sweep, s)):
                dn_copy(sweep, s).wait_recv()
            gain(top, OMEGA * COUPLE * unpack(dn_in[sweep, s], s), s)

    def arrive(outer, s, k):
        own = pl.ds(pl.multiple_of(k * nodes, nodes), nodes)
        with scope("wlat%d" % s):
            lat_copy(outer, s, k, (p + 1) % lat_count).wait_recv()
        gain(own, OMEGA * COUPLE * unpack(lat_in[outer, s, k], s), s)
        round_u(own)
        return own

    def close(sweep, s, acc):
        take(sweep, s)
        apply_h(sweep, s)
        apply_dn(sweep, s)

    def send_next(sweep, s, acc):
        with scope("sendnext%d" % s):
            low = acc[lower, :] + product(lower, lower)
            send_low(sweep, s, lambda rows: low[rows.start - 4 * nodes : rows.stop - 4 * nodes, :])

    def advance_all(acc):
        for block in blocks(every):
            total = acc[block, :] + product(block, lower)
            u[block, :] = u[block, :] + OMEGA * left_over(block, total)

    def bulk_rows(acc, s):
        add(acc, upper, upper)
        for block in blocks(upper):
            gain(block, OMEGA * left_over(block, acc[block, :]), s)
        round_u(upper)

    load_face.wait()
    load_code.wait()
    for k in SEND_ORDER:
        make_hot(k)
    with scope("loadu"):
        load_u.wait()
    with scope("mkf"):
        for k in SEND_ORDER:
            face = oriented(k)
            for s in HALVES:
                lat_out[0, s, k] = pack(face, s)
            if k == SEND_ORDER[0]:
                with scope("bar"):
                    pl.semaphore_wait(barrier, len(offsets) + inner)
            lat_copy(0, 0, k, lat_target(k)).start()
        for k in SEND_ORDER:
            lat_copy(0, 1, k, lat_target(k)).start()
    round_u(every)
    load_diag.wait()
    for block in range(6 * nodes // lanes):
        own = slice(block * lanes, (block + 1) * lanes)
        diag[own, :] = jnp.broadcast_to(diag_row[:, own], (lanes, lanes)).T
    with scope("waitw"):
        load_rhs.wait()
        load_factor.wait()
        for copy in load_w:
            copy.wait()
    for s in HALVES:
        packed_factor[s] = pack(factor[...], s)
    ahead, behind = sums.at[0], sums.at[1]
    with scope("acc0"):
        for block in blocks(every):
            u[block, :] = u[block, :] + OMEGA * left_over(block, product(block, every))

    near = lax.rem(p, 2)
    order = (1 - near, 2, 3, near)
    for outer in range(ITERS):
        first, second = outer * RADIAL_PASSES, outer * RADIAL_PASSES + 1
        round_u(lower)
        if outer < ITERS - 1:
            with scope("lacc"):
                for block in blocks(every):
                    moved = product(block, lower)
                    ahead[block, :] = moved
                    behind[block, :] = moved
            for s, acc in enumerate((ahead, behind)):
                for turn, k in enumerate(order):
                    own = arrive(outer, s, k)
                    add(acc, lower, own)
                    if s == 1 and turn == 0:
                        relay(second_layer, first, 0)
                with scope("sendlow%d" % s):
                    send_low(first, s, lambda rows: acc[rows, :])
                if s == 0:
                    with scope("bulkA"):
                        bulk_rows(acc, s)
                        begin(acc, every, upper)
            relay(later_layer, first, 0)
            for s, acc in enumerate((ahead, behind)):
                if s == 1:
                    with scope("bulkB1"):
                        bulk_rows(acc, s)
                    relay(second_layer, first, 1)
                    with scope("bulkB2"):
                        begin(acc, every, upper)
                    relay(later_layer, first, 1)
                close(first, s, acc)
                with scope("fin%d" % s):
                    round_u(lower)
                    for block in blocks(upper):
                        gain(block, OMEGA * left_over(block, acc[block, :] + product(block, lower)), s)
                if s == 1:
                    send_next(second, s, acc)
                    relay(second_layer, second, 0)
                with scope("faces%d" % s):
                    send_faces(outer + 1, s)
                if s == 0:
                    send_next(second, s, acc)
            relay(later_layer, second, 0)
            relay(inner_layer, second, 1)
            with scope("bulk3"):
                round_u(upper)
                begin(behind, every, upper)
            for s in HALVES:
                close(second, s, behind)
            with scope("bulk4"):
                round_u(lower)
                advance_all(behind)
        else:
            with scope("lacc"):
                begin(behind, lower, lower)
            for s in HALVES:
                for k in order:
                    arrive(outer, s, k)
                acc = ahead if s == 0 else behind
                for block in blocks(lower):
                    acc[block, :] = behind[block, :] + product(block, upper)
                with scope("sendlow%d" % s):
                    send_low(first, s, lambda rows: acc[rows, :])
            relay(second_layer, first, 0)
            with scope("bulk1"):
                for block in blocks(upper):
                    total = product(block, every)
                    u[block, :] = u[block, :] + OMEGA * left_over(block, total)
                round_u(upper)
            with scope("bulk2"):
                begin(behind, lower, upper)
            relay(later_layer, first, 0)
            relay(inner_layer, first, 1)
            for s in HALVES:
                close(first, s, behind)
                round_half(lower, s)
                send_next(second, s, behind)
                relay(second_layer, second, s)
    with scope("lastup"):
        for block in blocks(upper):
            u[block, :] = u[block, :] + OMEGA * left_over(block, product(block, every))
    final = ITERS * RADIAL_PASSES - 1
    stores = [
        pltpu.make_async_copy(u.at[part], out_hbm.at[0, 0, part], out_sem.at[n])
        for n, part in enumerate((upper, bottom, top))
    ]
    stores[0].start()
    for s in HALVES:
        relay(later_layer, final, s)
        take(final, s)
        apply_h(final, s)
    stores[1].start()
    for s in HALVES:
        apply_dn(final, s)
    stores[2].start()

    with scope("wsend"):
        for outer in range(ITERS):
            lat_sent(outer).wait_send()

        @pl.when(r > 0)
        def _():
            for sweep in range(ITERS * RADIAL_PASSES):
                dn_sent(sweep).wait_send()

        @pl.when(r < rad_count - 1)
        def _():
            for sweep in range(ITERS * RADIAL_PASSES):
                h_sent(sweep).wait_send()

    with scope("wout"):
        for copy in stores:
            copy.wait()


def per_device(lat_count, rad_count, schur_off, schur_diag, source, start, decay, neighbour_face, orientation):
    order, columns = source.shape[2:]
    nodes = order // 6
    sweeps = ITERS * RADIAL_PASSES
    patches, contacts = neighbour_face.shape
    faces = lambda *lead: pltpu.VMEM((*lead, nodes, columns), jnp.float32)
    packed = lambda *lead: pltpu.VMEM((*lead, 2, nodes // 2, columns), jnp.float32)
    wide = lambda dtype: pltpu.VMEM((order, columns), dtype)
    dma = lambda *shape: pltpu.SemaphoreType.DMA(shape)
    hbm = pl.BlockSpec(memory_space=pltpu.HBM)
    return pl.pallas_call(
        functools.partial(kernel, lat_count, rad_count, nodes),
        out_shape=jax.ShapeDtypeStruct(source.shape, jnp.float32),
        in_specs=[hbm] * 7,
        out_specs=pl.BlockSpec(memory_space=pl.ANY),
        scratch_shapes=[
            pltpu.SMEM((contacts, patches), jnp.int32),
            pltpu.SMEM((contacts, patches), jnp.int32),
            pltpu.VMEM((1, order), jnp.float32),
            pltpu.VMEM((order, order), jnp.bfloat16),
            wide(jnp.float32),
            wide(jnp.bfloat16),
            wide(jnp.float32),
            faces(),
            wide(jnp.float32),
            pltpu.VMEM((2, order, columns), jnp.float32),
            packed(),
            packed(),
            pltpu.VMEM((4, nodes, nodes), jnp.bfloat16),
            pltpu.VMEM((ITERS, 2, 4, nodes // 2, columns), jnp.float32),
            pltpu.VMEM((ITERS, 2, 4, nodes // 2, columns), jnp.float32),
            packed(sweeps), packed(sweeps), packed(sweeps), packed(sweeps),
            dma(3), dma(3), dma(2), dma(3),
            dma(ITERS), dma(ITERS, 2, 4), dma(sweeps), dma(2, 2),
            dma(sweeps), dma(2, 2, CHUNKS),
        ],
        compiler_params=pltpu.CompilerParams(
            collective_id=0, has_side_effects=True, vmem_limit_bytes=24 * 1024 * 1024
        ),
        name="shell",
    )(*(
        pltpu.with_memory_space_constraint(x, pltpu.HBM)
        for x in (neighbour_face.T, orientation.T, schur_diag, schur_off, source, start, decay)
    ))


def solution(mesh):
    lat_count, rad_count = mesh.shape["lat"], mesh.shape["rad"]
    return jax.shard_map(
        functools.partial(per_device, lat_count, rad_count),
        mesh=mesh,
        in_specs=(
            P("lat", "rad", None, None),
            P("lat", "rad", None),
            P("lat", "rad", None, None),
            P("lat", "rad", None, None),
            P("lat", "rad", None, None),
            P(),
            P(),
        ),
        out_specs=P("lat", "rad", None, None),
        check_vma=False,
    )
```

```python
import contextlib
import functools
import math

import jax
import jax.numpy as jnp
from jax import lax
from jax.experimental import pallas as pl
from jax.experimental.pallas import tpu as pltpu
from jax.sharding import PartitionSpec as P

ITERS = 2
RADIAL_PASSES = 2
OMEGA = 0.3
COUPLE = 0.5
CHUNKS = 8
HALVES = (0, 1)
SEND_ORDER = (2, 3, 0, 1)
MESH = pl.DeviceIdType.MESH


def scope(name):
    return contextlib.nullcontext()


def one_hot(code, side):
    nodes = side * side
    n = lax.broadcasted_iota(jnp.int32, (nodes, 1), 0)
    i, j = n // side, n % side
    swap, rows, cols = code & 1, (code >> 1) & 1, (code >> 2) & 1
    a = i + swap * (j - i)
    b = j + swap * (i - j)
    a = a + rows * (side - 1 - 2 * a)
    b = b + cols * (side - 1 - 2 * b)
    at = lax.broadcasted_iota(jnp.int32, (nodes, nodes), 1)
    return jnp.where(at == a * side + b, 1.0, 0.0).astype(jnp.bfloat16)


def permuted(hot, face):
    high = face.astype(jnp.bfloat16)
    rest = face - high.astype(jnp.float32)
    middle = rest.astype(jnp.bfloat16)
    low = (rest - middle.astype(jnp.float32)).astype(jnp.bfloat16)
    total = None
    for part in (low, middle, high):
        moved = jnp.dot(hot, part, preferred_element_type=jnp.float32)
        total = moved if total is None else total + moved
    return total


def kernel(
    lat_count, rad_count, nodes,
    face_hbm, code_hbm, diag_hbm, w_hbm, source_hbm, start_hbm, decay_hbm,
    out_hbm,
    face_at, code_at, diag_row, w, u, ub, rhs, factor, diag, sums, packed_factor, packed_top, hot,
    lat_out, lat_in, dn_out, dn_in, h_out, h_in,
    small_sem, load_sem, w_sem, out_sem,
    lat_send, lat_recv, dn_send, dn_recv, h_send, h_recv,
):
    side = math.isqrt(nodes)
    far = max(2, lat_count // 8)
    offsets = (-1, 1, -far, far)
    p = lax.axis_index("lat")
    r = lax.axis_index("rad")
    lanes = u.shape[1]
    half = lanes // 2
    size = nodes // 2 // CHUNKS
    upper, lower, every = slice(0, 4 * nodes), slice(4 * nodes, 6 * nodes), slice(0, 6 * nodes)
    bottom, top = slice(4 * nodes, 5 * nodes), slice(5 * nodes, 6 * nodes)

    load_face = pltpu.make_async_copy(face_hbm, face_at, small_sem.at[0])
    load_code = pltpu.make_async_copy(code_hbm, code_at, small_sem.at[1])
    load_diag = pltpu.make_async_copy(diag_hbm.at[0], diag_row, small_sem.at[2])
    load_u = pltpu.make_async_copy(start_hbm.at[0, 0], u, load_sem.at[0])
    load_rhs = pltpu.make_async_copy(source_hbm.at[0, 0], rhs, load_sem.at[1])
    load_factor = pltpu.make_async_copy(decay_hbm.at[0, 0], factor, load_sem.at[2])
    load_w = [
        pltpu.make_async_copy(w_hbm.at[0, 0, part], w.at[part], w_sem.at[n])
        for n, part in enumerate((upper, lower))
    ]
    load_face.start()
    load_code.start()
    load_u.start()

    barrier = pltpu.get_barrier_semaphore()
    for offset in offsets:
        target = (p - offset + lat_count) % lat_count
        pl.semaphore_signal(barrier, inc=1, device_id={"lat": target}, device_id_type=MESH)

    below, above = (r - 1 + rad_count) % rad_count, (r + 1) % rad_count
    first_layer, last_layer = r == 0, r == rad_count - 1
    inner_layer = jnp.logical_and(r > 0, r < rad_count - 1)
    second_layer = jnp.logical_and(r == 1, r < rad_count - 1)
    later_layer = jnp.logical_and(r > 1, r < rad_count - 1)

    @pl.when(r > 0)
    def _():
        pl.semaphore_signal(barrier, inc=1, device_id={"rad": below}, device_id_type=MESH)

    @pl.when(r < rad_count - 1)
    def _():
        pl.semaphore_signal(barrier, inc=1, device_id={"rad": above}, device_id_type=MESH)

    load_diag.start()
    for copy in load_w:
        copy.start()
    load_rhs.start()
    load_factor.start()

    inner = (r + rad_count - 1) // rad_count + (2 * rad_count - 2 - r) // rad_count

    def in_half(s, rows):
        lane = lax.broadcasted_iota(jnp.int32, (rows, lanes), 1)
        return lane < half if s == 0 else lane >= half

    def pack(x, s):
        first, second = x[: nodes // 2, :], x[nodes // 2 :, :]
        left = in_half(0, nodes // 2)
        if s == 0:
            return jnp.where(left, first, pltpu.roll(second, half, 1))
        return jnp.where(left, pltpu.roll(first, half, 1), second)

    def unpack(x, s):
        moved = pltpu.roll(x, half, 1)
        return jnp.concatenate([x, moved] if s == 0 else [moved, x], axis=0)

    def gain(rows, value, s):
        u[rows, :] = u[rows, :] + jnp.where(in_half(s, value.shape[0]), value, 0.0)

    def lat_copy(outer, s, k, target):
        return pltpu.make_async_remote_copy(
            src_ref=lat_out.at[outer, s, k], dst_ref=lat_in.at[outer, s, k],
            send_sem=lat_send.at[0], recv_sem=lat_recv.at[outer, s, k],
            device_id={"lat": target}, device_id_type=MESH,
        )

    def lat_target(k):
        return (p - offsets[k] + lat_count) % lat_count

    def lat_sent():
        return pltpu.make_async_remote_copy(
            src_ref=lat_out, dst_ref=lat_in,
            send_sem=lat_send.at[0], recv_sem=lat_recv.at[0, 0, 0],
            device_id={"lat": (p + 1) % lat_count}, device_id_type=MESH,
        )

    def dn_copy(sweep, s):
        return pltpu.make_async_remote_copy(
            src_ref=dn_out.at[sweep, s], dst_ref=dn_in.at[sweep, s],
            send_sem=dn_send.at[0], recv_sem=dn_recv.at[sweep % 2, s],
            device_id={"rad": below}, device_id_type=MESH,
        )

    def dn_sent():
        return pltpu.make_async_remote_copy(
            src_ref=dn_out, dst_ref=dn_in,
            send_sem=dn_send.at[0], recv_sem=dn_recv.at[0, 0],
            device_id={"rad": below}, device_id_type=MESH,
        )

    def h_copy(sweep, s, c):
        rows = pl.ds(c * size, size)
        return pltpu.make_async_remote_copy(
            src_ref=h_out.at[sweep, s, rows], dst_ref=h_in.at[sweep, s, rows],
            send_sem=h_send.at[0], recv_sem=h_recv.at[sweep % 2, s, c],
            device_id={"rad": above}, device_id_type=MESH,
        )

    def h_sent():
        return pltpu.make_async_remote_copy(
            src_ref=h_out, dst_ref=h_in,
            send_sem=h_send.at[0], recv_sem=h_recv.at[0, 0, 0],
            device_id={"rad": above}, device_id_type=MESH,
        )

    def make_hot(k):
        hot[k] = one_hot(code_at[k, lat_target(k)], side)

    def oriented(k):
        which = jnp.full((nodes, lanes), face_at[k, lat_target(k)], jnp.int32)
        face = u[slice(0, nodes), :]
        for f in range(1, 4):
            face = jnp.where(which == f, u[slice(f * nodes, (f + 1) * nodes), :], face)
        return permuted(hot[k], face)

    def send_faces(outer, s):
        for pair in (SEND_ORDER[:2], SEND_ORDER[2:]):
            faces = [pack(oriented(k), s) for k in pair]
            for k, face in zip(pair, faces):
                lat_out[outer, s, k] = face
            for k in pair:
                lat_copy(outer, s, k, lat_target(k)).start()

    def product(rows, columns):
        return jnp.dot(w[rows, columns], ub[columns, :], preferred_element_type=jnp.float32)

    def blocks(rows):
        return [slice(at, at + nodes) for at in range(rows.start, rows.stop, nodes)]

    def add(acc, rows, columns):
        for block in blocks(rows):
            acc[block, :] = acc[block, :] + product(block, columns)

    def begin(acc, rows, columns):
        for block in blocks(rows):
            acc[block, :] = product(block, columns)

    def left_over(rows, total):
        return rhs[rows, :] - (total + diag[rows, :] * u[rows, :])

    def round_u(rows):
        ub[rows, :] = u[rows, :].astype(jnp.bfloat16)

    def round_half(rows, s):
        count = rows.stop - rows.start
        old = ub[rows, :].astype(jnp.float32)
        ub[rows, :] = jnp.where(in_half(s, count), u[rows, :], old).astype(jnp.bfloat16)

    def send_low(sweep, s, total):
        res = left_over(bottom, total(bottom))
        dn_out[sweep, s] = pack(res, s)

        @pl.when(r > 0)
        def _():
            dn_copy(sweep, s).start()

        gain(bottom, OMEGA * res, s)
        res = left_over(top, total(top))
        packed_top[s] = pack(res, s)

        @pl.when(first_layer)
        def _():
            h_out[sweep, s] = packed_factor[s] * packed_top[s]
            for c in range(CHUNKS):
                h_copy(sweep, s, c).start()

        gain(top, OMEGA * res, s)

    def relay(where, sweep, s):
        @pl.when(where)
        def _():
            with scope("relay%d%d" % (sweep, s)):
                for c in range(CHUNKS):
                    rows = slice(c * size, (c + 1) * size)
                    h_copy(sweep, s, c).wait_recv()
                    h_out[sweep, s, rows] = packed_factor[s, rows] * (
                        h_in[sweep, s, rows] + packed_top[s, rows]
                    )
                    h_copy(sweep, s, c).start()

    def take(sweep, s):
        @pl.when(last_layer)
        def _():
            with scope("take%d%d" % (sweep, s)):
                for c in range(CHUNKS):
                    h_copy(sweep, s, c).wait_recv()

    def apply_h(sweep, s):
        @pl.when(r > 0)
        def _():
            gain(bottom, OMEGA * COUPLE * unpack(h_in[sweep, s], s), s)

    def apply_dn(sweep, s):
        @pl.when(r < rad_count - 1)
        def _():
            with scope("wdn%d%d" % (sweep, s)):
                dn_copy(sweep, s).wait_recv()
            gain(top, OMEGA * COUPLE * unpack(dn_in[sweep, s], s), s)

    def arrive(outer, s, k):
        own = pl.ds(pl.multiple_of(k * nodes, nodes), nodes)
        with scope("wlat%d" % s):
            lat_copy(outer, s, k, (p + 1) % lat_count).wait_recv()
        gain(own, OMEGA * COUPLE * unpack(lat_in[outer, s, k], s), s)
        round_u(own)
        return own

    def close(sweep, s, acc):
        take(sweep, s)
        apply_h(sweep, s)
        apply_dn(sweep, s)

    def send_next(sweep, s, acc):
        with scope("sendnext%d" % s):
            low = acc[lower, :] + product(lower, lower)
            send_low(sweep, s, lambda rows: low[rows.start - 4 * nodes : rows.stop - 4 * nodes, :])

    def advance_all(acc):
        for block in blocks(every):
            total = acc[block, :] + product(block, lower)
            u[block, :] = u[block, :] + OMEGA * left_over(block, total)

    def bulk_rows(acc, s):
        add(acc, upper, upper)
        for block in blocks(upper):
            gain(block, OMEGA * left_over(block, acc[block, :]), s)
        round_u(upper)

    load_face.wait()
    load_code.wait()
    for k in SEND_ORDER:
        make_hot(k)
    with scope("loadu"):
        load_u.wait()
    with scope("mkf"):
        for k in SEND_ORDER:
            face = oriented(k)
            for s in HALVES:
                lat_out[0, s, k] = pack(face, s)
            if k == SEND_ORDER[0]:
                with scope("bar"):
                    pl.semaphore_wait(barrier, len(offsets) + inner)
            lat_copy(0, 0, k, lat_target(k)).start()
        for k in SEND_ORDER:
            lat_copy(0, 1, k, lat_target(k)).start()
    round_u(every)
    load_diag.wait()
    for block in range(6 * nodes // lanes):
        own = slice(block * lanes, (block + 1) * lanes)
        diag[own, :] = jnp.broadcast_to(diag_row[:, own], (lanes, lanes)).T
    with scope("waitw"):
        load_rhs.wait()
        load_factor.wait()
        for copy in load_w:
            copy.wait()
    for s in HALVES:
        packed_factor[s] = pack(factor[...], s)
    ahead, behind = sums.at[0], sums.at[1]
    with scope("acc0"):
        for block in blocks(every):
            u[block, :] = u[block, :] + OMEGA * left_over(block, product(block, every))

    near = lax.rem(p, 2)
    order = (1 - near, 2, 3, near)
    for outer in range(ITERS):
        first, second = outer * RADIAL_PASSES, outer * RADIAL_PASSES + 1
        round_u(lower)
        if outer < ITERS - 1:
            with scope("lacc"):
                for block in blocks(every):
                    moved = product(block, lower)
                    ahead[block, :] = moved
                    behind[block, :] = moved
            for s, acc in enumerate((ahead, behind)):
                for turn, k in enumerate(order):
                    own = arrive(outer, s, k)
                    add(acc, lower, own)
                    if s == 1 and turn == 0:
                        relay(second_layer, first, 0)
                with scope("sendlow%d" % s):
                    send_low(first, s, lambda rows: acc[rows, :])
                if s == 0:
                    with scope("bulkA"):
                        bulk_rows(acc, s)
                        begin(acc, every, upper)
            relay(later_layer, first, 0)
            for s, acc in enumerate((ahead, behind)):
                if s == 1:
                    with scope("bulkB1"):
                        bulk_rows(acc, s)
                    relay(second_layer, first, 1)
                    with scope("bulkB2"):
                        begin(acc, every, upper)
                    relay(later_layer, first, 1)
                close(first, s, acc)
                round_u(lower)
                if s == 1:
                    send_next(second, s, acc)
                    relay(second_layer, second, 0)
                with scope("fin%d" % s):
                    for block in blocks(upper):
                        gain(block, OMEGA * left_over(block, acc[block, :] + product(block, lower)), s)
                with scope("faces%d" % s):
                    send_faces(outer + 1, s)
                if s == 0:
                    send_next(second, s, acc)
            relay(later_layer, second, 0)
            relay(inner_layer, second, 1)
            with scope("bulk3"):
                round_u(upper)
                begin(behind, every, upper)
            for s in HALVES:
                close(second, s, behind)
            with scope("bulk4"):
                round_u(lower)
                advance_all(behind)
        else:
            with scope("lacc"):
                begin(behind, lower, lower)
            for s in HALVES:
                for k in order:
                    arrive(outer, s, k)
                acc = ahead if s == 0 else behind
                for block in blocks(lower):
                    acc[block, :] = behind[block, :] + product(block, upper)
                with scope("sendlow%d" % s):
                    send_low(first, s, lambda rows: acc[rows, :])
            relay(second_layer, first, 0)
            with scope("bulk1"):
                for block in blocks(upper):
                    total = product(block, every)
                    u[block, :] = u[block, :] + OMEGA * left_over(block, total)
                round_u(upper)
            with scope("bulk2"):
                begin(behind, lower, upper)
            relay(later_layer, first, 0)
            relay(inner_layer, first, 1)
            for s in HALVES:
                close(first, s, behind)
                round_half(lower, s)
                send_next(second, s, behind)
            for s in HALVES:
                relay(second_layer, second, s)
    with scope("lastup"):
        for block in blocks(upper):
            u[block, :] = u[block, :] + OMEGA * left_over(block, product(block, every))
    final = ITERS * RADIAL_PASSES - 1
    stores = [
        pltpu.make_async_copy(u.at[part], out_hbm.at[0, 0, part], out_sem.at[0])
        for part in (upper, bottom, top)
    ]
    stores[0].start()
    for s in HALVES:
        relay(later_layer, final, s)
        take(final, s)
        apply_h(final, s)
    stores[1].start()
    for s in HALVES:
        apply_dn(final, s)
    stores[2].start()

    with scope("wsend"):
        lat_sent().wait_send()

        @pl.when(r > 0)
        def _():
            dn_sent().wait_send()

        @pl.when(r < rad_count - 1)
        def _():
            h_sent().wait_send()

    with scope("wout"):
        pltpu.make_async_copy(u, out_hbm.at[0, 0], out_sem.at[0]).wait()


def per_device(lat_count, rad_count, schur_off, schur_diag, source, start, decay, neighbour_face, orientation):
    order, columns = source.shape[2:]
    nodes = order // 6
    sweeps = ITERS * RADIAL_PASSES
    patches, contacts = neighbour_face.shape
    faces = lambda *lead: pltpu.VMEM((*lead, nodes, columns), jnp.float32)
    packed = lambda *lead: pltpu.VMEM((*lead, 2, nodes // 2, columns), jnp.float32)
    wide = lambda dtype: pltpu.VMEM((order, columns), dtype)
    dma = lambda *shape: pltpu.SemaphoreType.DMA(shape)
    hbm = pl.BlockSpec(memory_space=pltpu.HBM)
    return pl.pallas_call(
        functools.partial(kernel, lat_count, rad_count, nodes),
        out_shape=jax.ShapeDtypeStruct(source.shape, jnp.float32),
        in_specs=[hbm] * 7,
        out_specs=pl.BlockSpec(memory_space=pl.ANY),
        scratch_shapes=[
            pltpu.SMEM((contacts, patches), jnp.int32),
            pltpu.SMEM((contacts, patches), jnp.int32),
            pltpu.VMEM((1, order), jnp.float32),
            pltpu.VMEM((order, order), jnp.bfloat16),
            wide(jnp.float32),
            wide(jnp.bfloat16),
            wide(jnp.float32),
            faces(),
            wide(jnp.float32),
            pltpu.VMEM((2, order, columns), jnp.float32),
            packed(),
            packed(),
            pltpu.VMEM((4, nodes, nodes), jnp.bfloat16),
            pltpu.VMEM((ITERS, 2, 4, nodes // 2, columns), jnp.float32),
            pltpu.VMEM((ITERS, 2, 4, nodes // 2, columns), jnp.float32),
            packed(sweeps), packed(sweeps), packed(sweeps), packed(sweeps),
            dma(3), dma(3), dma(2), dma(1),
            dma(1), dma(ITERS, 2, 4), dma(1), dma(2, 2),
            dma(1), dma(2, 2, CHUNKS),
        ],
        compiler_params=pltpu.CompilerParams(
            collective_id=0, has_side_effects=True, vmem_limit_bytes=24 * 1024 * 1024
        ),
        name="shell",
    )(*(
        pltpu.with_memory_space_constraint(x, pltpu.HBM)
        for x in (neighbour_face.T, orientation.T, schur_diag, schur_off, source, start, decay)
    ))


def solution(mesh):
    lat_count, rad_count = mesh.shape["lat"], mesh.shape["rad"]
    return jax.shard_map(
        functools.partial(per_device, lat_count, rad_count),
        mesh=mesh,
        in_specs=(
            P("lat", "rad", None, None),
            P("lat", "rad", None),
            P("lat", "rad", None, None),
            P("lat", "rad", None, None),
            P("lat", "rad", None, None),
            P(),
            P(),
        ),
        out_specs=P("lat", "rad", None, None),
        check_vma=False,
    )
```

```python
import contextlib
import functools
import math

import jax
import jax.numpy as jnp
from jax import lax
from jax.experimental import pallas as pl
from jax.experimental.pallas import tpu as pltpu
from jax.sharding import PartitionSpec as P

ITERS = 2
RADIAL_PASSES = 2
OMEGA = 0.3
COUPLE = 0.5
CHUNKS = 8
HALVES = (0, 1)
MESH = pl.DeviceIdType.MESH


def scope(name):
    return contextlib.nullcontext()


def one_hot(code, side):
    nodes = side * side
    n = lax.broadcasted_iota(jnp.int32, (nodes, 1), 0)
    i, j = n // side, n % side
    swap, rows, cols = code & 1, (code >> 1) & 1, (code >> 2) & 1
    a = i + swap * (j - i)
    b = j + swap * (i - j)
    a = a + rows * (side - 1 - 2 * a)
    b = b + cols * (side - 1 - 2 * b)
    at = lax.broadcasted_iota(jnp.int32, (nodes, nodes), 1)
    return jnp.where(at == a * side + b, 1.0, 0.0).astype(jnp.bfloat16)


def permuted(hot, face):
    high = face.astype(jnp.bfloat16)
    rest = face - high.astype(jnp.float32)
    middle = rest.astype(jnp.bfloat16)
    low = (rest - middle.astype(jnp.float32)).astype(jnp.bfloat16)
    total = None
    for part in (low, middle, high):
        moved = jnp.dot(hot, part, preferred_element_type=jnp.float32)
        total = moved if total is None else total + moved
    return total


def kernel(
    lat_count, rad_count, nodes,
    face_hbm, code_hbm, diag_hbm, w_hbm, source_hbm, start_hbm, decay_hbm,
    out_hbm,
    face_at, code_at, diag_row, w, u, ub, rhs, factor, diag, sums, packed_factor, packed_top, hot,
    lat_out, lat_in, dn_out, dn_in, h_out, h_in,
    small_sem, load_sem, w_sem, out_sem,
    lat_send, lat_recv, dn_send, dn_recv, h_send, h_recv,
):
    side = math.isqrt(nodes)
    far = max(2, lat_count // 8)
    offsets = (-1, 1, -far, far)
    p = lax.axis_index("lat")
    r = lax.axis_index("rad")
    lanes = u.shape[1]
    half = lanes // 2
    size = nodes // 2 // CHUNKS
    upper, lower, every = slice(0, 4 * nodes), slice(4 * nodes, 6 * nodes), slice(0, 6 * nodes)
    bottom, top = slice(4 * nodes, 5 * nodes), slice(5 * nodes, 6 * nodes)

    load_face = pltpu.make_async_copy(face_hbm, face_at, small_sem.at[0])
    load_code = pltpu.make_async_copy(code_hbm, code_at, small_sem.at[1])
    load_diag = pltpu.make_async_copy(diag_hbm.at[0], diag_row, small_sem.at[2])
    load_u = pltpu.make_async_copy(start_hbm.at[0, 0], u, load_sem.at[0])
    load_rhs = pltpu.make_async_copy(source_hbm.at[0, 0], rhs, load_sem.at[1])
    load_factor = pltpu.make_async_copy(decay_hbm.at[0, 0], factor, load_sem.at[2])
    load_w = [
        pltpu.make_async_copy(w_hbm.at[0, 0, part], w.at[part], w_sem.at[n])
        for n, part in enumerate((upper, lower))
    ]
    load_face.start()
    load_code.start()
    load_u.start()

    barrier = pltpu.get_barrier_semaphore()
    for offset in offsets:
        target = (p - offset + lat_count) % lat_count
        pl.semaphore_signal(barrier, inc=1, device_id={"lat": target}, device_id_type=MESH)

    below, above = (r - 1 + rad_count) % rad_count, (r + 1) % rad_count
    first_layer, last_layer = r == 0, r == rad_count - 1
    inner_layer = jnp.logical_and(r > 0, r < rad_count - 1)
    second_layer = jnp.logical_and(r == 1, r < rad_count - 1)
    later_layer = jnp.logical_and(r > 1, r < rad_count - 1)

    @pl.when(r > 0)
    def _():
        pl.semaphore_signal(barrier, inc=1, device_id={"rad": below}, device_id_type=MESH)

    @pl.when(r < rad_count - 1)
    def _():
        pl.semaphore_signal(barrier, inc=1, device_id={"rad": above}, device_id_type=MESH)

    load_diag.start()
    for copy in load_w:
        copy.start()
    load_rhs.start()
    load_factor.start()

    inner = (r + rad_count - 1) // rad_count + (2 * rad_count - 2 - r) // rad_count

    def in_half(s, rows):
        lane = lax.broadcasted_iota(jnp.int32, (rows, lanes), 1)
        return lane < half if s == 0 else lane >= half

    def pack(x, s):
        first, second = x[: nodes // 2, :], x[nodes // 2 :, :]
        left = in_half(0, nodes // 2)
        if s == 0:
            return jnp.where(left, first, pltpu.roll(second, half, 1))
        return jnp.where(left, pltpu.roll(first, half, 1), second)

    def unpack(x, s):
        moved = pltpu.roll(x, half, 1)
        return jnp.concatenate([x, moved] if s == 0 else [moved, x], axis=0)

    def gain(rows, value, s):
        u[rows, :] = u[rows, :] + jnp.where(in_half(s, value.shape[0]), value, 0.0)

    def lat_copy(outer, s, k, target):
        return pltpu.make_async_remote_copy(
            src_ref=lat_out.at[outer, s, k], dst_ref=lat_in.at[outer, s, k],
            send_sem=lat_send.at[0], recv_sem=lat_recv.at[outer, s, k],
            device_id={"lat": target}, device_id_type=MESH,
        )

    def lat_target(k):
        reach = 1 + (k // 2) * (far - 1)
        return (p - (2 * (k % 2) - 1) * reach + lat_count) % lat_count

    def lat_sent():
        return pltpu.make_async_remote_copy(
            src_ref=lat_out, dst_ref=lat_in,
            send_sem=lat_send.at[0], recv_sem=lat_recv.at[0, 0, 0],
            device_id={"lat": (p + 1) % lat_count}, device_id_type=MESH,
        )

    def dn_copy(sweep, s):
        return pltpu.make_async_remote_copy(
            src_ref=dn_out.at[sweep, s], dst_ref=dn_in.at[sweep, s],
            send_sem=dn_send.at[0], recv_sem=dn_recv.at[sweep % 2, s],
            device_id={"rad": below}, device_id_type=MESH,
        )

    def dn_sent():
        return pltpu.make_async_remote_copy(
            src_ref=dn_out, dst_ref=dn_in,
            send_sem=dn_send.at[0], recv_sem=dn_recv.at[0, 0],
            device_id={"rad": below}, device_id_type=MESH,
        )

    def h_copy(sweep, s, c):
        rows = pl.ds(c * size, size)
        return pltpu.make_async_remote_copy(
            src_ref=h_out.at[sweep, s, rows], dst_ref=h_in.at[sweep, s, rows],
            send_sem=h_send.at[0], recv_sem=h_recv.at[sweep % 2, s, c],
            device_id={"rad": above}, device_id_type=MESH,
        )

    def h_sent():
        return pltpu.make_async_remote_copy(
            src_ref=h_out, dst_ref=h_in,
            send_sem=h_send.at[0], recv_sem=h_recv.at[0, 0, 0],
            device_id={"rad": above}, device_id_type=MESH,
        )

    near, pair = lax.rem(p, 2), lax.rem(p // 2, 2)
    send_order = (2 + pair, 3 - pair, 1 - near, near)
    order = (1 - near, 3 - pair, 2 + pair, near)

    def make_hot(k):
        hot[k] = one_hot(code_at[k, lat_target(k)], side)

    def oriented(k):
        which = jnp.full((nodes, lanes), face_at[k, lat_target(k)], jnp.int32)
        face = u[slice(0, nodes), :]
        for f in range(1, 4):
            face = jnp.where(which == f, u[slice(f * nodes, (f + 1) * nodes), :], face)
        return permuted(hot[k], face)

    def send_faces(outer, s):
        for some in (send_order[:2], send_order[2:]):
            faces = [pack(oriented(k), s) for k in some]
            for k, face in zip(some, faces):
                lat_out[outer, s, k] = face
            for k in some:
                lat_copy(outer, s, k, lat_target(k)).start()

    def product(rows, columns):
        return jnp.dot(w[rows, columns], ub[columns, :], preferred_element_type=jnp.float32)

    def blocks(rows):
        return [slice(at, at + nodes) for at in range(rows.start, rows.stop, nodes)]

    def add(acc, rows, columns):
        for block in blocks(rows):
            acc[block, :] = acc[block, :] + product(block, columns)

    def begin(acc, rows, columns):
        for block in blocks(rows):
            acc[block, :] = product(block, columns)

    def left_over(rows, total):
        return rhs[rows, :] - (total + diag[rows, :] * u[rows, :])

    def round_u(rows):
        ub[rows, :] = u[rows, :].astype(jnp.bfloat16)

    def round_half(rows, s):
        count = rows.stop - rows.start
        old = ub[rows, :].astype(jnp.float32)
        ub[rows, :] = jnp.where(in_half(s, count), u[rows, :], old).astype(jnp.bfloat16)

    def send_low(sweep, s, total):
        res = left_over(bottom, total(bottom))
        dn_out[sweep, s] = pack(res, s)

        @pl.when(r > 0)
        def _():
            dn_copy(sweep, s).start()

        gain(bottom, OMEGA * res, s)
        res = left_over(top, total(top))
        packed_top[s] = pack(res, s)

        @pl.when(first_layer)
        def _():
            h_out[sweep, s] = packed_factor[s] * packed_top[s]
            for c in range(CHUNKS):
                h_copy(sweep, s, c).start()

        gain(top, OMEGA * res, s)

    def relay(where, sweep, s):
        @pl.when(where)
        def _():
            with scope("relay%d%d" % (sweep, s)):
                for c in range(CHUNKS):
                    rows = slice(c * size, (c + 1) * size)
                    h_copy(sweep, s, c).wait_recv()
                    h_out[sweep, s, rows] = packed_factor[s, rows] * (
                        h_in[sweep, s, rows] + packed_top[s, rows]
                    )
                    h_copy(sweep, s, c).start()

    def take(sweep, s):
        @pl.when(last_layer)
        def _():
            with scope("take%d%d" % (sweep, s)):
                for c in range(CHUNKS):
                    h_copy(sweep, s, c).wait_recv()

    def apply_h(sweep, s):
        @pl.when(r > 0)
        def _():
            gain(bottom, OMEGA * COUPLE * unpack(h_in[sweep, s], s), s)

    def apply_dn(sweep, s):
        @pl.when(r < rad_count - 1)
        def _():
            with scope("wdn%d%d" % (sweep, s)):
                dn_copy(sweep, s).wait_recv()
            gain(top, OMEGA * COUPLE * unpack(dn_in[sweep, s], s), s)

    def arrive(outer, s, k):
        own = pl.ds(pl.multiple_of(k * nodes, nodes), nodes)
        with scope("wlat%d" % s):
            lat_copy(outer, s, k, (p + 1) % lat_count).wait_recv()
        gain(own, OMEGA * COUPLE * unpack(lat_in[outer, s, k], s), s)
        round_u(own)
        return own

    def close(sweep, s, acc):
        take(sweep, s)
        apply_h(sweep, s)
        apply_dn(sweep, s)

    def send_next(sweep, s, acc):
        with scope("sendnext%d" % s):
            low = acc[lower, :] + product(lower, lower)
            send_low(sweep, s, lambda rows: low[rows.start - 4 * nodes : rows.stop - 4 * nodes, :])

    def advance_half(acc, s):
        round_half(lower, s)
        for block in blocks(every):
            total = acc[block, :] + product(block, lower)
            gain(block, OMEGA * left_over(block, total), s)
        round_half(lower, s)

    def bulk_rows(acc, s):
        add(acc, upper, upper)
        for block in blocks(upper):
            gain(block, OMEGA * left_over(block, acc[block, :]), s)
        round_u(upper)

    load_face.wait()
    load_code.wait()
    for k in range(len(offsets)):
        make_hot(k)
    with scope("loadu"):
        load_u.wait()
    with scope("mkf"):
        for n, k in enumerate(send_order):
            face = oriented(k)
            for s in HALVES:
                lat_out[0, s, k] = pack(face, s)
            if n == 0:
                with scope("bar"):
                    pl.semaphore_wait(barrier, len(offsets) + inner)
            lat_copy(0, 0, k, lat_target(k)).start()
        for k in send_order:
            lat_copy(0, 1, k, lat_target(k)).start()
    round_u(every)
    load_diag.wait()
    for block in range(6 * nodes // lanes):
        own = slice(block * lanes, (block + 1) * lanes)
        diag[own, :] = jnp.broadcast_to(diag_row[:, own], (lanes, lanes)).T
    with scope("waitw"):
        load_rhs.wait()
        load_factor.wait()
        for copy in load_w:
            copy.wait()
    for s in HALVES:
        packed_factor[s] = pack(factor[...], s)
    ahead, behind = sums.at[0], sums.at[1]
    with scope("acc0"):
        for block in blocks(every):
            u[block, :] = u[block, :] + OMEGA * left_over(block, product(block, every))

    for outer in range(ITERS):
        first, second = outer * RADIAL_PASSES, outer * RADIAL_PASSES + 1
        if outer < ITERS - 1:
            round_u(lower)
            with scope("lacc"):
                for block in blocks(every):
                    moved = product(block, lower)
                    ahead[block, :] = moved
                    behind[block, :] = moved
            for s, acc in enumerate((ahead, behind)):
                for turn, k in enumerate(order):
                    own = arrive(outer, s, k)
                    add(acc, lower, own)
                    if s == 1 and turn == 0:
                        relay(second_layer, first, 0)
                with scope("sendlow%d" % s):
                    send_low(first, s, lambda rows: acc[rows, :])
                if s == 0:
                    with scope("bulkA"):
                        bulk_rows(acc, s)
                        begin(acc, every, upper)
            relay(later_layer, first, 0)
            for s, acc in enumerate((ahead, behind)):
                if s == 1:
                    with scope("bulkB1"):
                        bulk_rows(acc, s)
                    relay(second_layer, first, 1)
                    with scope("bulkB2"):
                        begin(acc, every, upper)
                    relay(later_layer, first, 1)
                close(first, s, acc)
                round_u(lower)
                if s == 1:
                    send_next(second, s, acc)
                    relay(second_layer, second, 0)
                with scope("fin%d" % s):
                    for block in blocks(upper):
                        gain(block, OMEGA * left_over(block, acc[block, :] + product(block, lower)), s)
                with scope("faces%d" % s):
                    send_faces(outer + 1, s)
                if s == 0:
                    send_next(second, s, acc)
            relay(later_layer, second, 0)
            relay(inner_layer, second, 1)
            with scope("bulk3"):
                round_u(upper)
                begin(behind, every, upper)
        else:
            for s in HALVES:
                close(first - 1, s, behind)
                with scope("bulk4"):
                    advance_half(behind, s)
                acc = ahead
                with scope("lacc"):
                    begin(acc, lower, lower)
                for k in order:
                    arrive(outer, s, k)
                add(acc, lower, upper)
                with scope("sendlow%d" % s):
                    send_low(first, s, lambda rows: acc[rows, :])
            relay(second_layer, first, 0)
            with scope("bulk1"):
                for block in blocks(upper):
                    total = product(block, every)
                    u[block, :] = u[block, :] + OMEGA * left_over(block, total)
                round_u(upper)
            with scope("bulk2"):
                begin(behind, lower, upper)
            relay(later_layer, first, 0)
            relay(inner_layer, first, 1)
            for s in HALVES:
                close(first, s, behind)
                round_half(lower, s)
                send_next(second, s, behind)
            for s in HALVES:
                relay(second_layer, second, s)
    with scope("lastup"):
        for block in blocks(upper):
            u[block, :] = u[block, :] + OMEGA * left_over(block, product(block, every))
    final = ITERS * RADIAL_PASSES - 1
    stores = [
        pltpu.make_async_copy(u.at[part], out_hbm.at[0, 0, part], out_sem.at[0])
        for part in (upper, bottom, top)
    ]
    stores[0].start()
    for s in HALVES:
        relay(later_layer, final, s)
        take(final, s)
        apply_h(final, s)
    stores[1].start()
    for s in HALVES:
        apply_dn(final, s)
    stores[2].start()

    with scope("wsend"):
        lat_sent().wait_send()

        @pl.when(r > 0)
        def _():
            dn_sent().wait_send()

        @pl.when(r < rad_count - 1)
        def _():
            h_sent().wait_send()

    with scope("wout"):
        pltpu.make_async_copy(u, out_hbm.at[0, 0], out_sem.at[0]).wait()


def per_device(lat_count, rad_count, schur_off, schur_diag, source, start, decay, neighbour_face, orientation):
    order, columns = source.shape[2:]
    nodes = order // 6
    sweeps = ITERS * RADIAL_PASSES
    patches, contacts = neighbour_face.shape
    faces = lambda *lead: pltpu.VMEM((*lead, nodes, columns), jnp.float32)
    packed = lambda *lead: pltpu.VMEM((*lead, 2, nodes // 2, columns), jnp.float32)
    wide = lambda dtype: pltpu.VMEM((order, columns), dtype)
    dma = lambda *shape: pltpu.SemaphoreType.DMA(shape)
    hbm = pl.BlockSpec(memory_space=pltpu.HBM)
    return pl.pallas_call(
        functools.partial(kernel, lat_count, rad_count, nodes),
        out_shape=jax.ShapeDtypeStruct(source.shape, jnp.float32),
        in_specs=[hbm] * 7,
        out_specs=pl.BlockSpec(memory_space=pl.ANY),
        scratch_shapes=[
            pltpu.SMEM((contacts, patches), jnp.int32),
            pltpu.SMEM((contacts, patches), jnp.int32),
            pltpu.VMEM((1, order), jnp.float32),
            pltpu.VMEM((order, order), jnp.bfloat16),
            wide(jnp.float32),
            wide(jnp.bfloat16),
            wide(jnp.float32),
            faces(),
            wide(jnp.float32),
            pltpu.VMEM((2, order, columns), jnp.float32),
            packed(),
            packed(),
            pltpu.VMEM((4, nodes, nodes), jnp.bfloat16),
            pltpu.VMEM((ITERS, 2, 4, nodes // 2, columns), jnp.float32),
            pltpu.VMEM((ITERS, 2, 4, nodes // 2, columns), jnp.float32),
            packed(sweeps), packed(sweeps), packed(sweeps), packed(sweeps),
            dma(3), dma(3), dma(2), dma(1),
            dma(1), dma(ITERS, 2, 4), dma(1), dma(2, 2),
            dma(1), dma(2, 2, CHUNKS),
        ],
        compiler_params=pltpu.CompilerParams(
            collective_id=0, has_side_effects=True, vmem_limit_bytes=24 * 1024 * 1024
        ),
        name="shell",
    )(*(
        pltpu.with_memory_space_constraint(x, pltpu.HBM)
        for x in (neighbour_face.T, orientation.T, schur_diag, schur_off, source, start, decay)
    ))


def solution(mesh):
    lat_count, rad_count = mesh.shape["lat"], mesh.shape["rad"]
    return jax.shard_map(
        functools.partial(per_device, lat_count, rad_count),
        mesh=mesh,
        in_specs=(
            P("lat", "rad", None, None),
            P("lat", "rad", None),
            P("lat", "rad", None, None),
            P("lat", "rad", None, None),
            P("lat", "rad", None, None),
            P(),
            P(),
        ),
        out_specs=P("lat", "rad", None, None),
        check_vma=False,
    )
```
